256 devices in a mesh: row: 8 (over z_hi, core), col: 8 (over y, z_lo), depth: 4 (over x).
Axes of the slice: x: 4, y: 4, z: 8 (z_hi: 4, z_lo: 2; z = z_hi * 2 + z_lo), core: 2. Of those that a mesh axis runs over, the one named last changes fastest.
Arguments:
- factor: float32 [32768, 1536], P(('row', 'col', 'depth')), may hold values from -1 to 4, as said below
- update: float32 [32768, 256], P(('row', 'col', 'depth')), may hold values from -0.375 to 0.375
Outputs:
- new_factor: float32 [32768, 1536], P(('row', 'col', 'depth'))
- new_update: float32 [32768, 256], P(('row', 'col', 'depth'))
The draws below stay inside these ranges and needn't reach their ends.
Inputs may be any that keep to these rules, and one draw needn't show every extreme that they name: `factor`: zero above the diagonal; each diagonal entry is 1 or more.
All inputs are finite; a program needn't handle non-finite values.
Results may differ from the reference program's by a relative error of at most 0.00013.
Values sent between devices are 32-bit elements; how exact they have to be, the bound alone decides.
No kernel may reach another device: no remote copies, remote signals or barrier semaphores. Data moves between devices by JAX's collectives and lax.ppermute only.
A program may use at most 128 MiB of HBM per device.

```python
import math
import jax
import jax.numpy as jnp
from jax import lax

B = 512
K = 256
PANELS = 3
N = 32768
WIN = 1536


def draw_factor(key, part):
    key_off, key_diag = jax.random.split(key)
    row_ids = jnp.arange(N, dtype=jnp.int32)[:, None]
    col_ids = jnp.arange(WIN, dtype=jnp.int32)[None, :]
    lower_part = jax.random.normal(key_off, (N, WIN), jnp.float32) / math.sqrt(B)
    diagonal = jax.random.uniform(key_diag, (WIN,), jnp.float32, 1.0, 2.0)
    lower_part = jnp.clip(lower_part, -0.9, 0.9)
    return jnp.where(row_ids > col_ids, lower_part, jnp.where(row_ids == col_ids, diagonal[None, :], jnp.float32(0.0)))


def level_of(own_key, shape, pieces, least, high):
    level, own = 1.0, jax.random.fold_in(own_key, 6)
    for position, blocks in pieces:
        steps = jnp.exp(jax.random.uniform(jax.random.fold_in(own, position), (blocks,), jnp.float32, least / len(pieces), high / len(pieces)))
        level = level * jnp.repeat(steps, shape[position] // blocks).reshape([-1 if axis == position else 1 for axis in range(len(shape))])
    return level


def noise(key, dims, scale, most, cuts=(), kind=jnp.bfloat16):
    loudness = level_of(key, dims, cuts, -0.22, 0.18) if cuts else 1.0
    drawn = jax.random.normal(key, dims, jnp.float32) * scale * loudness
    return jnp.minimum(jnp.maximum(drawn, -most), most).astype(kind)


def setup_inputs(seed: int = 0) -> dict:
    streams_of = jax.random.split(jax.random.key(seed), 3)
    factor = draw_factor(jax.random.fold_in(streams_of[2], 71), 0)
    update = noise(streams_of[1], (N, K), 0.0625, 0.375, ((0, 256),), jnp.float32)
    return dict(factor=factor, update=update)


def transform(stacked):
    panel_width = stacked.shape[0]
    diag_block = stacked[:, :panel_width]
    v_block = stacked[:, panel_width:]
    update_rank = v_block.shape[1]
    gram_matrix = jnp.dot(stacked, stacked.T, precision=lax.Precision.HIGHEST)
    new_diag = jnp.linalg.cholesky(gram_matrix)
    leading = jax.scipy.linalg.solve_triangular(new_diag, stacked, lower=True)
    coupling = jax.scipy.linalg.solve_triangular(diag_block, v_block, lower=True)
    identity_k = jnp.eye(update_rank, dtype=jnp.float32)
    inner_gram = identity_k + jnp.dot(coupling.T, coupling, precision=lax.Precision.HIGHEST)
    lower_inner = jnp.linalg.cholesky(inner_gram)
    null_basis = jnp.concatenate([-coupling, identity_k], 0)
    second = jax.scipy.linalg.solve_triangular(lower_inner, null_basis.T, lower=True).T
    return jnp.concatenate([leading.T, second], 1)

def reference(factor, update):
    row_ids = jnp.arange(N, dtype=jnp.int32)
    for panel_index in range(PANELS):
        panel_start = panel_index * B
        panel_cols = factor[:, panel_start:panel_start + B]
        stacked = jnp.concatenate([panel_cols, update], 1)
        rotation = transform(stacked[panel_start:panel_start + B])
        moved = jnp.dot(stacked, rotation, precision=lax.Precision.HIGHEST)
        col_ids = panel_start + jnp.arange(B, dtype=jnp.int32)
        new_cols = jnp.where(row_ids[:, None] >= col_ids[None, :], moved[:, :B], jnp.float32(0.0))
        update = jnp.where(row_ids[:, None] >= panel_start, moved[:, B:], update)
        factor = factor.at[:, panel_start:panel_start + B].set(new_cols)
    return (factor, update)
```

```python
import jax
import jax.numpy as jnp
from jax import lax
from jax.experimental import pallas as pl
from jax.experimental.pallas import tpu as pltpu
from jax.sharding import PartitionSpec as P

B = 512
K = 256
PANELS = 3
BLK = 128
STEP = 16
AXES = ("row", "col", "depth")
HI = lax.Precision.HIGHEST
F32 = jnp.float32


def nn(a, b):
    return lax.dot_general(a, b, (((1,), (0,)), ((), ())), precision=HI, preferred_element_type=F32)


def nt(a, b):
    return lax.dot_general(a, b, (((1,), (1,)), ((), ())), precision=HI, preferred_element_type=F32)


def iota(shape, dim):
    return lax.broadcasted_iota(jnp.int32, shape, dim)


def tri_inverse_128(blocks):
    r = iota((BLK, BLK), 0)
    c = iota((BLK, BLK), 1)
    inv = [jnp.where(r == c, 1.0 / jnp.where(r == c, d, 1.0), 0.0) for d in blocks]
    m = 1
    while m < BLK:
        pick = (r // (2 * m) == c // (2 * m)) & (r // m != c // m) & (r > c)
        low = [jnp.where(pick, d, 0.0) for d in blocks]
        if m == 1:
            mid = [jnp.sum(x, axis=0, keepdims=True) for x in inv]
            row = [jnp.sum(x, axis=1, keepdims=True) for x in inv]
            inv = [x - rr * l * mm for x, l, rr, mm in zip(inv, low, row, mid)]
        else:
            half = [nn(l, x) for l, x in zip(low, inv)]
            inv = [x - nn(x, h) for x, h in zip(inv, half)]
        m *= 2
    return inv


def gauss_step(blocks, j0):
    shape = (STEP, BLK)
    r = iota(shape, 0)
    c = iota(shape, 1)
    here = (c >= j0) & (c < j0 + STEP)
    eye = jnp.where(c == r + j0, 1.0, 0.0)
    rows = [w[j0 : j0 + STEP, :] for w in blocks]
    cols = [[jnp.broadcast_to(x[:, j0 + t : j0 + t + 1], shape) for t in range(STEP)] for x in rows]
    rest = [jnp.where(here, eye, x) for x in rows]
    lin = [jnp.zeros(shape, F32) for _ in rows]
    for t in range(STEP):
        at = r == t
        for i in range(len(blocks)):
            pivot = jnp.broadcast_to(cols[i][t][t : t + 1, :], shape)
            root = lax.rsqrt(pivot)
            recip = root * root
            mult = jnp.where(at, -recip, cols[i][t] * recip)
            lin[i] = jnp.where(at, rest[i] * root, lin[i])
            rest[i] = jnp.where(at, 0.0, rest[i]) - mult * rest[i][t : t + 1, :]
            for u in range(t + 1, STEP):
                cols[i][u] = jnp.where(at, 0.0, cols[i][u]) - mult * cols[i][u][t : t + 1, :]
    lin = [jnp.where(c < j0 + STEP, x, 0.0) for x in lin]
    return rest, lin


def chol_inverse_128(blocks):
    c = iota((BLK, BLK), 1)
    out = [[] for _ in blocks]
    for j in range(BLK // STEP):
        j0 = j * STEP
        rest, lin = gauss_step(blocks, j0)
        for i in range(len(blocks)):
            out[i].append(lin[i])
        if j0 + STEP < BLK:
            here = (c >= j0) & (c < j0 + STEP)
            blocks = [
                jnp.where(here, 0.0, w) - nn(w[:, j0 : j0 + STEP], z) for w, z in zip(blocks, rest)
            ]
    return [jnp.concatenate(x, 0) for x in out]


def eliminate(refs, nb):
    def step(k, carry):
        del carry
        start = pl.multiple_of(k * BLK, BLK)
        inv = chol_inverse_128([ref[k, pl.ds(start, BLK), :] for ref in refs])
        for ref, x in zip(refs, inv):
            ref[k] = nt(ref[k], x)

        def trail(l, carry):
            del carry
            first = pl.multiple_of(l * BLK, BLK)
            for ref in refs:
                ref[l] = ref[l] - nt(ref[k], ref[k, pl.ds(first, BLK), :])
            return 0

        lax.fori_loop(k + 1, nb, trail, 0)
        return 0

    lax.fori_loop(0, nb, step, 0)


def params():
    return pltpu.CompilerParams(vmem_limit_bytes=56 * 1024 * 1024)


def call(kernel, outs, scratch, scalars, *arrays):
    smem = pl.BlockSpec(memory_space=pltpu.SMEM)
    vmem = pl.BlockSpec(memory_space=pltpu.VMEM)
    return pl.pallas_call(
        kernel,
        out_shape=[jax.ShapeDtypeStruct(s, F32) for s in outs],
        in_specs=[smem] + [vmem] * len(arrays),
        out_specs=[vmem] * len(outs),
        scratch_shapes=[pltpu.VMEM(s, F32) for s in scratch],
        compiler_params=params(),
    )(scalars, *arrays)


def first_kernel(pos, d0, d1, d2, d3, u0, u1, u2, u3, inv_ref, v_ref, g_ref, d_s, u_s):
    depth = pos[0]
    for shift, (d, u) in enumerate(((d0, u0), (d1, u1), (d2, u2), (d3, u3))):
        slot = (depth + 4 - shift) % 4
        d_s[slot] = d[...]
        u_s[slot] = u[...]
    diag = tri_inverse_128([d_s[i, :, i * BLK : (i + 1) * BLK] for i in range(4)])
    low10 = -nn(diag[1], nn(d_s[1, :, 0:BLK], diag[0]))
    low32 = -nn(diag[3], nn(d_s[3, :, 2 * BLK : 3 * BLK], diag[2]))
    zero = jnp.zeros((BLK, BLK), F32)
    top = jnp.concatenate([jnp.concatenate([diag[0], zero], 1), jnp.concatenate([low10, diag[1]], 1)], 0)
    bot = jnp.concatenate([jnp.concatenate([diag[2], zero], 1), jnp.concatenate([low32, diag[3]], 1)], 0)
    below = jnp.concatenate([d_s[2, :, : 2 * BLK], d_s[3, :, : 2 * BLK]], 0)
    cross = -nn(bot, nn(below, top))
    inv_ref[0 : 2 * BLK, 0 : 2 * BLK] = top
    inv_ref[0 : 2 * BLK, 2 * BLK :] = jnp.zeros((2 * BLK, 2 * BLK), F32)
    inv_ref[2 * BLK :, 0 : 2 * BLK] = cross
    inv_ref[2 * BLK :, 2 * BLK :] = bot
    v = jnp.concatenate([u_s[i] for i in range(4)], 1)
    v_ref[...] = v
    g_ref[...] = nt(v, inv_ref[...])


def next_kernel(pos, g, l0, l1, l2, l3, v, inv, v_ref, g_ref, l_s):
    depth = pos[0]
    for shift, piece in enumerate((l0, l1, l2, l3)):
        l_s[(depth + 4 - shift) % 4] = piece[...]
    new = v[...] - nt(g[...], l_s[...].reshape(4 * BLK, B))
    v_ref[...] = new
    g_ref[...] = nt(new, inv[...])


def last_kernel(pos, f, u, a0, a1, a2, a3, o0, o1, o2, o3, f_ref, u_ref, t_s, h0, h1, h2, s0, s1, s2):
    depth, core, base = pos[0], pos[1], pos[2]
    for shift, (mine, other) in enumerate(((a0, o0), (a1, o1), (a2, o2), (a3, o3))):
        slot = (depth + 4 - shift) % 4
        t_s[slot * 2 + core] = mine[...]
        t_s[slot * 2 + 1 - core] = other[...]
    gt = [t_s[:, :, p * B : (p + 1) * B].reshape(K, B) for p in range(PANELS)]
    g = [x.T for x in gt]
    hs = (h0, h1, h2)
    ss = (s0, s1, s2)
    acc = jnp.where(iota((K, K), 0) == iota((K, K), 1), 1.0, 0.0)
    v = u[...]
    for p in range(PANELS):
        acc = acc + nt(gt[p], gt[p])
        v = v - nt(f[:, p * B : (p + 1) * B], gt[p])
        for k in range(2):
            sl = slice(k * BLK, (k + 1) * BLK)
            hs[p][k, 0:K, :] = acc[:, sl]
            hs[p][k, K : K + BLK, :] = v[:, sl]
            if p < PANELS - 1:
                hs[p][k, K + BLK :, :] = g[p + 1][:, sl]
    eliminate(hs, 2)
    before = [u[...]] + [
        jnp.concatenate([h[0, K : K + BLK, :], h[1, K : K + BLK, :]], 1) for h in hs
    ]
    turned = [g[0]] + [
        jnp.concatenate([h[0, K + BLK :, :], h[1, K + BLK :, :]], 1) for h in hs[:2]
    ]
    for p in range(PANELS):
        for k in range(4):
            part = turned[p][k * BLK : (k + 1) * BLK, :]
            eye = jnp.where(iota((B, BLK), 0) == iota((B, BLK), 1) + k * BLK, 1.0, 0.0)
            ss[p][k, 0:B, :] = eye + nt(turned[p], part)
            ss[p][k, B:, :] = f[:, p * B + k * BLK : p * B + (k + 1) * BLK] + nt(before[p], part)
    eliminate(ss, 4)
    rows = base + iota((BLK, BLK), 0)
    cols = iota((BLK, BLK), 1)
    for p in range(PANELS):
        for k in range(4):
            lo = p * B + k * BLK
            f_ref[:, lo : lo + BLK] = jnp.where(rows >= cols + lo, ss[p][k, B:, :], 0.0)
    rows = base + iota((BLK, K), 0)
    out = before[1]
    for p in range(1, PANELS):
        out = jnp.where(rows >= p * B, before[p + 1], out)
    u_ref[...] = out


def device(x, y, z, core):
    return (((z // 2) * 2 + core) * 8 + y * 2 + z % 2) * 4 + x


def owner(p, x):
    return p * 4 + x


def move(value, pairs):
    return lax.ppermute(value, AXES, pairs)


def depth_ring(shift):
    return [(owner(p, x), owner(p, (x + shift) % 4)) for p in range(PANELS) for x in range(4)]


def tree_steps():
    y0, z0 = 1, 0
    plans = (
        (("y", 2), ("y", 1), ("z", 4), ("z", 2), ("z", 1)),
        (("z", 4), ("z", 2), ("z", 1), ("y", 2), ("y", 1)),
    )
    held = [[(0, 0)], [(0, 0)]]
    for i in range(5):
        pairs = []
        for core in range(2):
            axis, hop = plans[core][i]
            new = []
            for dy, dz in held[core]:
                to = (dy + hop, dz) if axis == "y" else (dy, dz + hop)
                new.append(to)
                for x in range(4):
                    pairs.append(
                        (
                            device(x, (y0 + dy) % 4, (z0 + dz) % 8, core),
                            device(x, (y0 + to[0]) % 4, (z0 + to[1]) % 8, core),
                        )
                    )
            held[core] += new
        yield pairs


def everywhere(shift):
    return [((i // 4) * 4 + i % 4, (i // 4) * 4 + (i % 4 + shift) % 4) for i in range(256)]


def partner():
    return [
        (device(x, y, z, c), device(x, y, z, 1 - c))
        for x in range(4)
        for y in range(4)
        for z in range(8)
        for c in range(2)
    ]


def on_device(factor, update):
    row = lax.axis_index("row")
    depth = lax.axis_index("depth")
    core = row % 2
    flat = lax.axis_index(AXES)
    group = jnp.minimum(flat // 4, PANELS - 1)
    pos = jnp.stack([depth, core, flat * BLK]).astype(jnp.int32)

    own = lax.dynamic_slice(factor, (jnp.int32(0), group * B), (BLK, B))
    slices = update.T.reshape(4, K // 4, BLK)
    mine = lax.dynamic_index_in_dim(slices, depth, 0, keepdims=False)
    d_parts, u_parts = [own], [mine]
    for shift in range(1, 4):
        piece = lax.dynamic_index_in_dim(slices, (depth + shift) % 4, 0, keepdims=False)
        d_parts.append(move(own, depth_ring(shift)))
        u_parts.append(move(piece, depth_ring(shift)))
    left = [factor[:, :B]] + [move(factor[:, :B], depth_ring(s)) for s in range(1, 4)]
    left2 = [factor[:, B : 2 * B]] + [move(factor[:, B : 2 * B], depth_ring(s)[8:]) for s in range(1, 4)]

    inv, v, g0 = call(
        first_kernel,
        [(B, B), (K // 4, B), (K // 4, B)],
        [(4, BLK, B), (4, K // 4, BLK)],
        pos,
        *d_parts,
        *u_parts,
    )
    is0 = flat // 4 == 0
    is1 = flat // 4 == 1
    to1 = move(g0, [(owner(0, x), owner(1, x)) for x in range(4)])
    to2 = move(g0, [(owner(0, x), owner(2, x)) for x in range(4)])
    g0 = jnp.where(is0, g0, jnp.where(is1, to1, to2))
    v, g1 = call(next_kernel, [(K // 4, B), (K // 4, B)], [(4, BLK, B)], pos, g0, *left, v, inv)
    to2 = move(g1, [(owner(1, x), owner(2, x)) for x in range(4)])
    g1 = jnp.where(is1, g1, to2)
    _, g2 = call(next_kernel, [(K // 4, B), (K // 4, B)], [(4, BLK, B)], pos, g1, *left2, v, inv)

    quarter = jnp.concatenate([g0, g1, g2], 1)
    half = quarter[: K // 8]
    at_core1 = move(
        quarter[K // 8 :], [(device(x, 1, 0, 0), device(x, 1, 0, 1)) for x in range(4)]
    )
    half = jnp.where(core == 0, half, at_core1)
    for pairs in tree_steps():
        got = move(half, pairs)
        targets = jnp.zeros((256,), jnp.bool_).at[jnp.array([b for _, b in pairs])].set(True)
        half = jnp.where(targets[flat], got, half)
    mine = [half] + [move(half, everywhere(s)) for s in range(1, 4)]
    other = move(jnp.stack(mine), partner())
    return tuple(
        call(
            last_kernel,
            [factor.shape, update.shape],
            [
                (8, K // 8, PANELS * B),
                (2, K + BLK + B, BLK),
                (2, K + BLK + B, BLK),
                (2, K + BLK, BLK),
                (4, B + BLK, BLK),
                (4, B + BLK, BLK),
                (4, B + BLK, BLK),
            ],
            pos,
            factor,
            update,
            *mine,
            *[other[i] for i in range(4)],
        )
    )


def solution(mesh):
    spec = P(AXES, None)
    return jax.shard_map(
        on_device, mesh=mesh, in_specs=(spec, spec), out_specs=(spec, spec), check_vma=False
    )
```

```python
import jax
import jax.numpy as jnp
from jax import lax
from jax.experimental import pallas as pl
from jax.experimental.pallas import tpu as pltpu
from jax.sharding import PartitionSpec as P

B = 512
K = 256
PANELS = 3
BLK = 128
STEP = 16
NB = 6
AXES = ("row", "col", "depth")
PASSES = 6
GROUP = 1
F32 = jnp.float32


def pieces_of(x):
    terms = []
    for _ in range(2 if PASSES == 3 else 3):
        terms.append(x.astype(jnp.bfloat16))
        x = x - terms[-1].astype(F32)
    return terms


LEFT, RIGHT = ((0, 0, 1), (0, 1, 0)) if PASSES == 3 else ((0, 0, 0, 1, 1, 2), (0, 1, 2, 0, 1, 0))


def product(a, b, da, db):
    a = a if isinstance(a, list) else pieces_of(a)
    b = b if isinstance(b, list) else pieces_of(b)
    a = jnp.concatenate([a[i] for i in LEFT], da)
    b = jnp.concatenate([b[i] for i in RIGHT], db)
    return lax.dot_general(a, b, (((da,), (db,)), ((), ())), preferred_element_type=F32)


def nn(a, b):
    return product(a, b, 1, 0)


def nt(a, b):
    return product(a, b, 1, 1)


def tn(a, b):
    return product(a, b, 0, 0)


def iota(shape, dim):
    return lax.broadcasted_iota(jnp.int32, shape, dim)


def tri_inverse_128(blocks):
    r = iota((BLK, BLK), 0)
    c = iota((BLK, BLK), 1)
    inv = [jnp.where(r == c, 1.0 / jnp.where(r == c, d, 1.0), 0.0) for d in blocks]
    m = 1
    while m < BLK:
        pick = (r // (2 * m) == c // (2 * m)) & (r // m != c // m) & (r > c)
        low = [jnp.where(pick, d, 0.0) for d in blocks]
        if m == 1:
            mid = [jnp.sum(x, axis=0, keepdims=True) for x in inv]
            row = [jnp.sum(x, axis=1, keepdims=True) for x in inv]
            inv = [x - rr * l * mm for x, l, rr, mm in zip(inv, low, row, mid)]
        else:
            half = [nn(l, x) for l, x in zip(low, inv)]
            inv = [x - nn(x, h) for x, h in zip(inv, half)]
        m *= 2
    return inv


def row(x, s):
    return jnp.broadcast_to(x[s : s + 1, :], (8, BLK))


def col(x, c):
    return jnp.broadcast_to(x[:, c : c + 1], (8, BLK))


def cholesky_rows(tops, bots, j0):
    r = iota((8, BLK), 0)
    c = iota((8, BLK), 1)
    here = (c >= j0) & (c < j0 + STEP)
    n = range(len(tops))
    c0 = [[col(x, j0 + t) for t in range(8)] for x in tops]
    c1 = [[col(x, j0 + t) for t in range(STEP)] for x in bots]
    r0 = [jnp.where(here, jnp.where(c == r + j0, 1.0, 0.0), x) for x in tops]
    r1 = [jnp.where(here, jnp.where(c == r + j0 + 8, 1.0, 0.0), x) for x in bots]
    out0 = [None for _ in n]
    out1 = [None for _ in n]
    for t in range(STEP):
        s = t % 8
        at = r == s
        for i in n:
            if t < 8:
                root = lax.rsqrt(row(c0[i][t], s))
                recip = root * root
                m0 = c0[i][t] * recip
                m1 = c1[i][t] * recip
                for u in range(t + 1, 8):
                    x = row(c0[i][t], u)
                    c0[i][u] = c0[i][u] - m0 * x
                    c1[i][u] = c1[i][u] - m1 * x
                for u in range(8, STEP):
                    c1[i][u] = c1[i][u] - m1 * row(c1[i][t], u - 8)
                x = row(r0[i], s)
                done = x * root
                out0[i] = done if t == 0 else jnp.where(at, done, out0[i])
                r0[i] = r0[i] - m0 * x
                r1[i] = r1[i] - m1 * x
            else:
                root = lax.rsqrt(row(c1[i][t], s))
                m1 = c1[i][t] * (root * root)
                for u in range(t + 1, STEP):
                    c1[i][u] = c1[i][u] - m1 * row(c1[i][t], u - 8)
                x = row(r1[i], s)
                done = x * root
                out1[i] = done if t == 8 else jnp.where(at, done, out1[i])
                r1[i] = r1[i] - m1 * x
    return [jnp.concatenate([x, y], 0) for x, y in zip(out0, out1)]


def chol_inverse_128(src, dst, count):
    c = iota((STEP, BLK), 1)
    steps = BLK // STEP
    w = [[src[i, q * STEP : (q + 1) * STEP, :] for q in range(steps)] for i in range(count)]
    for j in range(steps):
        j0 = j * STEP
        for first in range(0, count, GROUP):
            some = range(first, min(first + GROUP, count))
            done = cholesky_rows([w[i][j][:8] for i in some], [w[i][j][8:] for i in some], j0)
            for i, x in zip(some, done):
                dst[i, j0 : j0 + STEP, :] = jnp.where(c < j0 + STEP, x, 0.0)
                if j + 1 < steps:
                    y = tn(x, x)
                    here = (c >= j0) & (c < j0 + STEP)
                    for q in range(j + 1, steps):
                        w[i][q] = jnp.where(here, 0.0, w[i][q]) - y[q * STEP : (q + 1) * STEP, :]


def call(kernel, mib, outs, scratch, scalars, *arrays):
    smem = pl.BlockSpec(memory_space=pltpu.SMEM)
    vmem = pl.BlockSpec(memory_space=pltpu.VMEM)
    outs = [s if isinstance(s, jax.ShapeDtypeStruct) else jax.ShapeDtypeStruct(s, F32) for s in outs]
    return pl.pallas_call(
        kernel,
        out_shape=outs,
        in_specs=[smem] + [vmem] * len(arrays),
        out_specs=[vmem] * len(outs),
        scratch_shapes=[pltpu.VMEM(s, F32) for s in scratch],
        compiler_params=pltpu.CompilerParams(vmem_limit_bytes=mib * 1024 * 1024),
    )(scalars, *arrays)


def pack_kernel(pos, f, u, p0, p1, p2, p3, left, u_s):
    depth, group = pos[0], pos[4]
    u_s[...] = u[...].T
    start = pl.multiple_of(group * B, B)
    for shift, out in enumerate((p0, p1, p2, p3)):
        for k in range(4):
            out[k * BLK : (k + 1) * BLK, :] = f[:, pl.ds(start + k * BLK, BLK)]
        first = pl.multiple_of(((depth + shift) % 4) * (K // 4), K // 4)
        out[4 * BLK :, :] = u_s[pl.ds(first, K // 4), :]
    left[...] = f[:, : 2 * B]


def first_kernel(pos, p0, p1, p2, p3, inv_ref, v_ref, g_ref, d_s):
    depth = pos[0]
    for shift, p in enumerate((p0, p1, p2, p3)):
        slot = (depth + 4 - shift) % 4
        d_s[slot] = p[: 4 * BLK, :].reshape(4, BLK, BLK)
        v_ref[slot] = p[4 * BLK :, :]
    diag = tri_inverse_128([d_s[i, i] for i in range(4)])
    low10 = -nn(diag[1], nn(d_s[1, 0], diag[0]))
    low32 = -nn(diag[3], nn(d_s[3, 2], diag[2]))
    zero = jnp.zeros((BLK, BLK), F32)
    top = jnp.concatenate([jnp.concatenate([diag[0], zero], 1), jnp.concatenate([low10, diag[1]], 1)], 0)
    bot = jnp.concatenate([jnp.concatenate([diag[2], zero], 1), jnp.concatenate([low32, diag[3]], 1)], 0)
    below = jnp.concatenate(
        [jnp.concatenate([d_s[i, 0], d_s[i, 1]], 1) for i in (2, 3)], 0
    )
    cross = -nn(bot, nn(below, top))
    inv = jnp.concatenate(
        [
            jnp.concatenate([top, jnp.zeros((2 * BLK, 2 * BLK), F32)], 1),
            jnp.concatenate([cross, bot], 1),
        ],
        0,
    )
    terms = pieces_of(inv)
    for i, x in enumerate(terms):
        inv_ref[i] = x
    v = jnp.concatenate([v_ref[i] for i in range(4)], 1)
    g_ref[...] = jnp.where(pos[3] == 0, nt(v, terms), 0.0)


def solve(pos, g, left, panel, v, inv, v_ref):
    depth = pos[0]
    terms = pieces_of(g)
    for shift, piece in enumerate(left):
        slot = (depth + 4 - shift) % 4
        v_ref[slot] = v[slot] - nt(terms, piece[:, (panel - 1) * B : panel * B])
    new = jnp.concatenate([v_ref[i] for i in range(4)], 1)
    return jnp.where(pos[3] == panel, nt(new, [inv[i] for i in range(3)]), 0.0)


def second_kernel(pos, own, got1, got2, l0, l1, l2, l3, v, inv, v_ref, sum_ref, g_ref):
    g = own[...] + got1[...] + got2[...]
    sum_ref[...] = g
    g_ref[...] = solve(pos, g, (l0, l1, l2, l3), 1, v, inv, v_ref)


def third_kernel(pos, g0, got, l0, l1, l2, l3, v, inv, half0_ref, half1_ref, v_s):
    g2 = solve(pos, got[...], (l0, l1, l2, l3), 2, v, inv, v_s)
    h = K // 8
    for ref, rows in ((half0_ref, slice(0, h)), (half1_ref, slice(h, 2 * h))):
        for i, g in enumerate((g0[...], got[...], g2)):
            ref[:, i * B : (i + 1) * B] = jnp.where(pos[3] == 2, g[rows], 0.0)


def last_kernel(pos, f, u, a0, a1, a2, a3, others, f_ref, u_ref, t_s, h_s, s_s, src, dst):
    depth, core, base = pos[0], pos[1], pos[2]
    for shift, mine in enumerate((a0, a1, a2, a3)):
        slot = (depth + 4 - shift) % 4
        t_s[slot * 2 + core] = mine[...]
        t_s[slot * 2 + 1 - core] = others[shift]
    acc = jnp.where(iota((K, K), 0) == iota((K, K), 1), 1.0, 0.0)
    v = u[...]
    for j in range(NB):
        gt = t_s[:, :, j * K : (j + 1) * K].reshape(K, K)
        acc = acc + nt(gt, gt)
        v = v - nt(f[:, j * K : (j + 1) * K], gt)
        for k in range(2):
            sl = slice(k * BLK, (k + 1) * BLK)
            h_s[j, k, 0:K, :] = acc[:, sl]
            h_s[j, k, K : K + BLK, :] = v[:, sl]
        g = gt.T
        if j == 0:
            first = g
        else:
            for k in range(2):
                h_s[j - 1, k, K + BLK :, :] = g[:, k * BLK : (k + 1) * BLK]

    def before(j):
        if j == 0:
            return u[...]
        return jnp.concatenate([h_s[j - 1, k, K : K + BLK, :] for k in range(2)], 1)

    def step(i, carry):
        del carry

        @pl.when(i == 0)
        def _():
            for j in range(NB):
                src[j] = h_s[j, 0, 0:BLK, :]

        chol_inverse_128(src, dst, NB)

        @pl.when(i == 0)
        def _():
            for j in range(NB):
                low = nt(h_s[j, 0, BLK:, :], dst[j])
                h_s[j, 0, BLK:, :] = low
                low = h_s[j, 1, BLK:, :] - nt(low, low[0:BLK, :])
                h_s[j, 1, BLK:, :] = low
                src[j] = low[0:BLK, :]

        @pl.when(i == 1)
        def _():
            for j in range(NB):
                h_s[j, 1, K:, :] = nt(h_s[j, 1, K:, :], dst[j])
            for j in range(NB):
                if j == 0:
                    g = first
                else:
                    g = jnp.concatenate([h_s[j - 1, k, K + BLK :, :] for k in range(2)], 1)
                full = nt(jnp.concatenate([g, before(j)], 0), g)
                eye = jnp.where(iota((K, K), 0) == iota((K, K), 1), 1.0, 0.0)
                s_s[j, 0:K, :] = full[0:K] + eye
                s_s[j, K:, :] = full[K:] + f[:, j * K : (j + 1) * K]
                src[j] = s_s[j, 0:BLK, 0:BLK]

        @pl.when(i == 2)
        def _():
            for j in range(NB):
                low = nt(s_s[j, BLK:, 0:BLK], dst[j])
                s_s[j, BLK:, 0:BLK] = low
                low = s_s[j, BLK:, BLK:] - nt(low, low[0:BLK, :])
                s_s[j, BLK:, BLK:] = low
                src[j] = low[0:BLK, :]

        @pl.when(i == 3)
        def _():
            rows = base + iota((BLK, BLK), 0)
            cols = iota((BLK, BLK), 1)
            for j in range(NB):
                lo = j * K
                f_ref[:, lo : lo + BLK] = jnp.where(rows >= cols + lo, s_s[j, K:, 0:BLK], 0.0)
                lo = lo + BLK
                new = nt(s_s[j, K:, BLK:], dst[j])
                f_ref[:, lo : lo + BLK] = jnp.where(rows >= cols + lo, new, 0.0)

        return 0

    lax.fori_loop(0, 4, step, 0)
    rows = base + iota((BLK, K), 0)
    out = before(2)
    for p in range(1, PANELS):
        out = jnp.where(rows >= p * B, before(2 * p + 2), out)
    u_ref[...] = out


def last_call(pos, factor, update, *pieces):
    return call(
        last_kernel,
        32,
        [factor.shape, update.shape],
        [
            (8, K // 8, PANELS * B),
            (NB, 2, K + BLK + K, BLK),
            (NB, K + BLK, K),
            (NB, BLK, BLK),
            (NB, BLK, BLK),
        ],
        pos,
        factor,
        update,
        *pieces,
    )


def device(x, y, z, core):
    return (((z // 2) * 2 + core) * 8 + y * 2 + z % 2) * 4 + x


def owner(p, x):
    return p * 4 + x


def move(value, pairs):
    return lax.ppermute(value, AXES, pairs)


def depth_ring(shift):
    return [(owner(p, x), owner(p, (x + shift) % 4)) for p in range(PANELS) for x in range(4)]


def tree_steps():
    y0, z0 = 1, 0
    plans = (
        (("y", 2), ("y", 1), ("z", 4), ("z", 2), ("z", 1)),
        (("z", 4), ("z", 2), ("z", 1), ("y", 2), ("y", 1)),
    )
    held = [[(0, 0)], [(0, 0)]]
    for i in range(5):
        pairs = []
        for core in range(2):
            axis, hop = plans[core][i]
            new = []
            for dy, dz in held[core]:
                to = (dy + hop, dz) if axis == "y" else (dy, dz + hop)
                new.append(to)
                for x in range(4):
                    pairs.append(
                        (
                            device(x, (y0 + dy) % 4, (z0 + dz) % 8, core),
                            device(x, (y0 + to[0]) % 4, (z0 + to[1]) % 8, core),
                        )
                    )
            held[core] += new
        yield pairs


def everywhere(shift):
    return [((i // 4) * 4 + i % 4, (i // 4) * 4 + (i % 4 + shift) % 4) for i in range(256)]


def partner():
    return [
        (device(x, y, z, c), device(x, y, z, 1 - c))
        for x in range(4)
        for y in range(4)
        for z in range(8)
        for c in range(2)
    ]


def on_device(factor, update):
    core = lax.axis_index("row") % 2
    depth = lax.axis_index("depth")
    flat = lax.axis_index(AXES)
    pos = jnp.stack([depth, core, flat * BLK, flat // 4, jnp.minimum(flat // 4, PANELS - 1)])
    pos = pos.astype(jnp.int32)
    quarter, half = K // 4, K // 8

    packed = (4 * BLK + quarter, BLK)
    p0, p1, p2, p3, left = call(
        pack_kernel, 8, [packed] * 4 + [(BLK, 2 * B)], [(K, BLK)], pos, factor, update
    )
    parts = [p0] + [move(p, depth_ring(s)) for s, p in ((1, p1), (2, p2), (3, p3))]
    left, *parts = lax.optimization_barrier((left, *parts))
    lefts = [left] + [move(left, depth_ring(s)[4:]) for s in range(1, 4)]
    inv, v, g0 = call(
        first_kernel,
        16,
        [jax.ShapeDtypeStruct((3, B, B), jnp.bfloat16), (4, quarter, BLK), (quarter, B)],
        [(4, 4, BLK, BLK)],
        pos,
        *parts,
    )
    got1 = move(g0, [(owner(0, x), owner(1, x)) for x in range(4)])
    got2 = move(g0, [(owner(0, x), owner(2, x)) for x in range(4)])
    v, g0, g1 = call(
        second_kernel,
        16,
        [(4, quarter, BLK), (quarter, B), (quarter, B)],
        [],
        pos,
        g0,
        got1,
        got2,
        *lefts,
        v,
        inv,
    )
    g1 = move(g1, [(owner(1, x), owner(2, x)) for x in range(4)])
    half0, half1 = call(
        third_kernel,
        16,
        [(half, PANELS * B)] * 2,
        [(4, quarter, BLK)],
        pos,
        g0,
        g1,
        *lefts,
        v,
        inv,
    )
    value = half0 + move(half1, [(device(x, 1, 0, 0), device(x, 1, 0, 1)) for x in range(4)])
    for pairs in tree_steps():
        value = value + move(value, pairs)
    mine = [value] + [move(value, everywhere(s)) for s in range(1, 4)]
    others = move(jnp.stack(mine), partner())
    return tuple(last_call(pos, factor, update, *mine, others))


def solution(mesh):
    spec = P(AXES, None)
    return jax.shard_map(
        on_device, mesh=mesh, in_specs=(spec, spec), out_specs=(spec, spec), check_vma=False
    )
```

```python
import jax
import jax.numpy as jnp
from jax import lax
from jax.experimental import pallas as pl
from jax.experimental.pallas import tpu as pltpu
from jax.sharding import PartitionSpec as P

B = 512
K = 256
PANELS = 3
BLK = 128
STEP = 16
NB = 6
AXES = ("row", "col", "depth")
PASSES = 6
SHARE = 16
F32 = jnp.float32


def pieces_of(x):
    terms = []
    for _ in range(2 if PASSES == 3 else 3):
        terms.append(x.astype(jnp.bfloat16))
        x = x - terms[-1].astype(F32)
    return terms


LEFT, RIGHT = ((0, 0, 1), (0, 1, 0)) if PASSES == 3 else ((0, 0, 0, 1, 1, 2), (0, 1, 2, 0, 1, 0))


def product(a, b, da, db):
    a = a if isinstance(a, list) else pieces_of(a)
    b = b if isinstance(b, list) else pieces_of(b)
    a = jnp.concatenate([a[i] for i in LEFT], da)
    b = jnp.concatenate([b[i] for i in RIGHT], db)
    return lax.dot_general(a, b, (((da,), (db,)), ((), ())), preferred_element_type=F32)


def nn(a, b):
    return product(a, b, 1, 0)


def nt(a, b):
    return product(a, b, 1, 1)


def tn(a, b):
    return product(a, b, 0, 0)


def iota(shape, dim):
    return lax.broadcasted_iota(jnp.int32, shape, dim)


def tri_inverse_128(blocks):
    r = iota((BLK, BLK), 0)
    c = iota((BLK, BLK), 1)
    inv = [jnp.where(r == c, 1.0 / jnp.where(r == c, d, 1.0), 0.0) for d in blocks]
    m = 1
    while m < BLK:
        pick = (r // (2 * m) == c // (2 * m)) & (r // m != c // m) & (r > c)
        low = [jnp.where(pick, d, 0.0) for d in blocks]
        if m == 1:
            mid = [jnp.sum(x, axis=0, keepdims=True) for x in inv]
            row = [jnp.sum(x, axis=1, keepdims=True) for x in inv]
            inv = [x - rr * l * mm for x, l, rr, mm in zip(inv, low, row, mid)]
        else:
            half = [nn(l, x) for l, x in zip(low, inv)]
            inv = [x - nn(x, h) for x, h in zip(inv, half)]
        m *= 2
    return inv


def row(x, s):
    return jnp.broadcast_to(x[s : s + 1, :], (8, BLK))


def col(x, c):
    return jnp.broadcast_to(x[:, c : c + 1], (8, BLK))


def cholesky_rows(blocks, j0):
    tiles = range(STEP // 8)
    shape = (8, BLK)
    r = iota(shape, 0)
    lane = iota(shape, 1)
    here = (lane >= j0) & (lane < j0 + STEP)
    x = [[w[8 * v : 8 * v + 8, :] for v in tiles] for w in blocks]
    part = [lane >= SHARE * i for i in range(len(blocks))]
    c = [[None] * (8 * v + 8) for v in tiles]
    for v in tiles:
        for t in range(8 * v + 8):
            both = col(x[0][v], j0 + t)
            for i in range(1, len(blocks)):
                both = jnp.where(part[i], col(x[i][v], j0 + t), both)
            c[v][t] = both
    mult = []
    roots = [None for _ in tiles]
    for t in range(STEP):
        first, s = divmod(t, 8)
        root = lax.rsqrt(row(c[first][t], s))
        recip = root * root
        m = {v: c[v][t] * recip for v in tiles if v >= first}
        m[first] = jnp.where(r > s, m[first], 0.0)
        for u in range(t + 1, STEP):
            y = row(c[u // 8][t], u % 8)
            for v in range(u // 8, len(tiles)):
                c[v][u] = c[v][u] - m[v] * y
        mult.append(m)
        roots[first] = root if s == 0 else jnp.where(r == s, root, roots[first])
    out = []
    for i, w in enumerate(x):
        rest = [jnp.where(here, jnp.where(lane == r + j0 + 8 * v, 1.0, 0.0), w[v]) for v in tiles]
        for t in range(STEP):
            first, s = divmod(t, 8)
            y = row(rest[first], s)
            for v, m in mult[t].items():
                rest[v] = rest[v] - col(m, SHARE * i) * y
        out.append(jnp.concatenate([rest[v] * col(roots[v], SHARE * i) for v in tiles], 0))
    return out


def chol_inverse_128(src, dst, count):
    c = iota((STEP, BLK), 1)
    steps = BLK // STEP
    w = [[src[i, q * STEP : (q + 1) * STEP, :] for q in range(steps)] for i in range(count)]
    for j in range(steps):
        j0 = j * STEP
        done = cholesky_rows([w[i][j] for i in range(count)], j0)
        for i, x in enumerate(done):
            dst[i, j0 : j0 + STEP, :] = jnp.where(c < j0 + STEP, x, 0.0)
            if j + 1 < steps:
                y = tn(x, x)
                here = (c >= j0) & (c < j0 + STEP)
                for q in range(j + 1, steps):
                    w[i][q] = jnp.where(here, 0.0, w[i][q]) - y[q * STEP : (q + 1) * STEP, :]


def call(kernel, mib, outs, scratch, scalars, *arrays):
    smem = pl.BlockSpec(memory_space=pltpu.SMEM)
    vmem = pl.BlockSpec(memory_space=pltpu.VMEM)
    outs = [s if isinstance(s, jax.ShapeDtypeStruct) else jax.ShapeDtypeStruct(s, F32) for s in outs]
    return pl.pallas_call(
        kernel,
        out_shape=outs,
        in_specs=[smem] + [vmem] * len(arrays),
        out_specs=[vmem] * len(outs),
        scratch_shapes=[pltpu.VMEM(s, F32) for s in scratch],
        compiler_params=pltpu.CompilerParams(vmem_limit_bytes=mib * 1024 * 1024),
    )(scalars, *arrays)


def pack_kernel(pos, f, u, p0, p1, p2, p3, left, u_s):
    depth, group = pos[0], pos[4]
    u_s[...] = u[...].T
    start = pl.multiple_of(group * B, B)
    for shift, out in enumerate((p0, p1, p2, p3)):
        for k in range(4):
            out[k * BLK : (k + 1) * BLK, :] = f[:, pl.ds(start + k * BLK, BLK)]
        first = pl.multiple_of(((depth + shift) % 4) * (K // 4), K // 4)
        out[4 * BLK :, :] = u_s[pl.ds(first, K // 4), :]
    left[...] = f[:, : 2 * B]


def first_kernel(pos, p0, p1, p2, p3, inv_ref, v_ref, g_ref, d_s):
    depth = pos[0]
    for shift, p in enumerate((p0, p1, p2, p3)):
        slot = (depth + 4 - shift) % 4
        d_s[slot] = p[: 4 * BLK, :].reshape(4, BLK, BLK)
        v_ref[slot] = p[4 * BLK :, :]
    diag = tri_inverse_128([d_s[i, i] for i in range(4)])
    low10 = -nn(diag[1], nn(d_s[1, 0], diag[0]))
    low32 = -nn(diag[3], nn(d_s[3, 2], diag[2]))
    zero = jnp.zeros((BLK, BLK), F32)
    top = jnp.concatenate([jnp.concatenate([diag[0], zero], 1), jnp.concatenate([low10, diag[1]], 1)], 0)
    bot = jnp.concatenate([jnp.concatenate([diag[2], zero], 1), jnp.concatenate([low32, diag[3]], 1)], 0)
    below = jnp.concatenate(
        [jnp.concatenate([d_s[i, 0], d_s[i, 1]], 1) for i in (2, 3)], 0
    )
    cross = -nn(bot, nn(below, top))
    inv = jnp.concatenate(
        [
            jnp.concatenate([top, jnp.zeros((2 * BLK, 2 * BLK), F32)], 1),
            jnp.concatenate([cross, bot], 1),
        ],
        0,
    )
    terms = pieces_of(inv)
    for i, x in enumerate(terms):
        inv_ref[i] = x
    v = jnp.concatenate([v_ref[i] for i in range(4)], 1)
    g_ref[...] = jnp.where(pos[3] == 0, nt(v, terms), 0.0)


def solve(pos, g, left, panel, v, inv, v_ref):
    depth = pos[0]
    terms = pieces_of(g)
    for shift, piece in enumerate(left):
        slot = (depth + 4 - shift) % 4
        v_ref[slot] = v[slot] - nt(terms, piece[:, (panel - 1) * B : panel * B])
    new = jnp.concatenate([v_ref[i] for i in range(4)], 1)
    return jnp.where(pos[3] == panel, nt(new, [inv[i] for i in range(3)]), 0.0)


def second_kernel(pos, own, got1, got2, l0, l1, l2, l3, v, inv, v_ref, sum_ref, g_ref):
    g = own[...] + got1[...] + got2[...]
    sum_ref[...] = g
    g_ref[...] = solve(pos, g, (l0, l1, l2, l3), 1, v, inv, v_ref)


def third_kernel(pos, g0, got, l0, l1, l2, l3, v, inv, half0_ref, half1_ref, v_s):
    g2 = solve(pos, got[...], (l0, l1, l2, l3), 2, v, inv, v_s)
    h = K // 8
    for ref, rows in ((half0_ref, slice(0, h)), (half1_ref, slice(h, 2 * h))):
        for i, g in enumerate((g0[...], got[...], g2)):
            ref[:, i * B : (i + 1) * B] = jnp.where(pos[3] == 2, g[rows], 0.0)


def last_kernel(pos, f, u, a0, a1, a2, a3, others, f_ref, u_ref, t_s, h_s, s_s, src, dst):
    depth, core, base = pos[0], pos[1], pos[2]
    for shift, mine in enumerate((a0, a1, a2, a3)):
        slot = (depth + 4 - shift) % 4
        t_s[slot * 2 + core] = mine[...]
        t_s[slot * 2 + 1 - core] = others[shift]
    acc = jnp.where(iota((K, K), 0) == iota((K, K), 1), 1.0, 0.0)
    v = u[...]
    for j in range(NB):
        gt = t_s[:, :, j * K : (j + 1) * K].reshape(K, K)
        acc = acc + nt(gt, gt)
        v = v - nt(f[:, j * K : (j + 1) * K], gt)
        for k in range(2):
            sl = slice(k * BLK, (k + 1) * BLK)
            h_s[j, k, 0:K, :] = acc[:, sl]
            h_s[j, k, K : K + BLK, :] = v[:, sl]
        g = gt.T
        if j == 0:
            first = g
        else:
            for k in range(2):
                h_s[j - 1, k, K + BLK :, :] = g[:, k * BLK : (k + 1) * BLK]

    def before(j):
        if j == 0:
            return u[...]
        return jnp.concatenate([h_s[j - 1, k, K : K + BLK, :] for k in range(2)], 1)

    def step(i, carry):
        del carry

        @pl.when(i == 0)
        def _():
            for j in range(NB):
                src[j] = h_s[j, 0, 0:BLK, :]

        chol_inverse_128(src, dst, NB)

        @pl.when(i == 0)
        def _():
            for j in range(NB):
                low = nt(h_s[j, 0, BLK:, :], dst[j])
                h_s[j, 0, BLK:, :] = low
                low = h_s[j, 1, BLK:, :] - nt(low, low[0:BLK, :])
                h_s[j, 1, BLK:, :] = low
                src[j] = low[0:BLK, :]

        @pl.when(i == 1)
        def _():
            for j in range(NB):
                h_s[j, 1, K:, :] = nt(h_s[j, 1, K:, :], dst[j])
            for j in range(NB):
                if j == 0:
                    g = first
                else:
                    g = jnp.concatenate([h_s[j - 1, k, K + BLK :, :] for k in range(2)], 1)
                full = nt(jnp.concatenate([g, before(j)], 0), g)
                eye = jnp.where(iota((K, K), 0) == iota((K, K), 1), 1.0, 0.0)
                s_s[j, 0:K, :] = full[0:K] + eye
                s_s[j, K:, :] = full[K:] + f[:, j * K : (j + 1) * K]
                src[j] = s_s[j, 0:BLK, 0:BLK]

        @pl.when(i == 2)
        def _():
            for j in range(NB):
                low = nt(s_s[j, BLK:, 0:BLK], dst[j])
                s_s[j, BLK:, 0:BLK] = low
                low = s_s[j, BLK:, BLK:] - nt(low, low[0:BLK, :])
                s_s[j, BLK:, BLK:] = low
                src[j] = low[0:BLK, :]

        @pl.when(i == 3)
        def _():
            rows = base + iota((BLK, BLK), 0)
            cols = iota((BLK, BLK), 1)
            for j in range(NB):
                lo = j * K
                f_ref[:, lo : lo + BLK] = jnp.where(rows >= cols + lo, s_s[j, K:, 0:BLK], 0.0)
                lo = lo + BLK
                new = nt(s_s[j, K:, BLK:], dst[j])
                f_ref[:, lo : lo + BLK] = jnp.where(rows >= cols + lo, new, 0.0)

        return 0

    lax.fori_loop(0, 4, step, 0)
    rows = base + iota((BLK, K), 0)
    out = before(2)
    for p in range(1, PANELS):
        out = jnp.where(rows >= p * B, before(2 * p + 2), out)
    u_ref[...] = out


def last_call(pos, factor, update, *pieces):
    return call(
        last_kernel,
        32,
        [factor.shape, update.shape],
        [
            (8, K // 8, PANELS * B),
            (NB, 2, K + BLK + K, BLK),
            (NB, K + BLK, K),
            (NB, BLK, BLK),
            (NB, BLK, BLK),
        ],
        pos,
        factor,
        update,
        *pieces,
    )


def device(x, y, z, core):
    return (((z // 2) * 2 + core) * 8 + y * 2 + z % 2) * 4 + x


def owner(p, x):
    return p * 4 + x


def move(value, pairs):
    return lax.ppermute(value, AXES, pairs)


def depth_ring(shift):
    return [(owner(p, x), owner(p, (x + shift) % 4)) for p in range(PANELS) for x in range(4)]


def tree_steps():
    y0, z0 = 1, 0
    plans = (
        (("y", 2), ("y", 1), ("z", 4), ("z", 2), ("z", 1)),
        (("z", 4), ("z", 2), ("z", 1), ("y", 2), ("y", 1)),
    )
    held = [[(0, 0)], [(0, 0)]]
    for i in range(5):
        pairs = []
        for core in range(2):
            axis, hop = plans[core][i]
            new = []
            for dy, dz in held[core]:
                to = (dy + hop, dz) if axis == "y" else (dy, dz + hop)
                new.append(to)
                for x in range(4):
                    pairs.append(
                        (
                            device(x, (y0 + dy) % 4, (z0 + dz) % 8, core),
                            device(x, (y0 + to[0]) % 4, (z0 + to[1]) % 8, core),
                        )
                    )
            held[core] += new
        yield pairs


def everywhere(shift):
    return [((i // 4) * 4 + i % 4, (i // 4) * 4 + (i % 4 + shift) % 4) for i in range(256)]


def partner():
    return [
        (device(x, y, z, c), device(x, y, z, 1 - c))
        for x in range(4)
        for y in range(4)
        for z in range(8)
        for c in range(2)
    ]


def on_device(factor, update):
    core = lax.axis_index("row") % 2
    depth = lax.axis_index("depth")
    flat = lax.axis_index(AXES)
    pos = jnp.stack([depth, core, flat * BLK, flat // 4, jnp.minimum(flat // 4, PANELS - 1)])
    pos = pos.astype(jnp.int32)
    quarter, half = K // 4, K // 8

    packed = (4 * BLK + quarter, BLK)
    p0, p1, p2, p3, left = call(
        pack_kernel, 8, [packed] * 4 + [(BLK, 2 * B)], [(K, BLK)], pos, factor, update
    )
    parts = [p0] + [move(p, depth_ring(s)) for s, p in ((1, p1), (2, p2), (3, p3))]
    inv, v, g0 = call(
        first_kernel,
        16,
        [jax.ShapeDtypeStruct((3, B, B), jnp.bfloat16), (4, quarter, BLK), (quarter, B)],
        [(4, 4, BLK, BLK)],
        pos,
        *parts,
    )
    left, g0 = lax.optimization_barrier((left, g0))
    got1 = move(g0, [(owner(0, x), owner(1, x)) for x in range(4)])
    got2 = move(g0, [(owner(0, x), owner(2, x)) for x in range(4)])
    lefts = [left] + [move(left, depth_ring(s)[4:]) for s in range(1, 4)]
    v, g0, g1 = call(
        second_kernel,
        16,
        [(4, quarter, BLK), (quarter, B), (quarter, B)],
        [],
        pos,
        g0,
        got1,
        got2,
        *lefts,
        v,
        inv,
    )
    g1 = move(g1, [(owner(1, x), owner(2, x)) for x in range(4)])
    half0, half1 = call(
        third_kernel,
        16,
        [(half, PANELS * B)] * 2,
        [(4, quarter, BLK)],
        pos,
        g0,
        g1,
        *lefts,
        v,
        inv,
    )
    value = half0 + move(half1, [(device(x, 1, 0, 0), device(x, 1, 0, 1)) for x in range(4)])
    for pairs in tree_steps():
        value = value + move(value, pairs)
    mine = [value] + [move(value, everywhere(s)) for s in range(1, 4)]
    others = move(jnp.stack(mine), partner())
    return tuple(last_call(pos, factor, update, *mine, others))


def solution(mesh):
    spec = P(AXES, None)
    return jax.shard_map(
        on_device, mesh=mesh, in_specs=(spec, spec), out_specs=(spec, spec), check_vma=False
    )
```

```python
import jax
import jax.numpy as jnp
from jax import lax
from jax.experimental import pallas as pl
from jax.experimental.pallas import tpu as pltpu
from jax.sharding import PartitionSpec as P

B = 512
K = 256
PANELS = 3
BLK = 128
STEP = 16
NB = 6
AXES = ("row", "col", "depth")
PASSES = 6
SHARE = 16
F32 = jnp.float32


def pieces_of(x):
    terms = []
    for _ in range(2 if PASSES == 3 else 3):
        terms.append(x.astype(jnp.bfloat16))
        x = x - terms[-1].astype(F32)
    return terms


LEFT, RIGHT = ((0, 0, 1), (0, 1, 0)) if PASSES == 3 else ((0, 0, 0, 1, 1, 2), (0, 1, 2, 0, 1, 0))


def product(a, b, da, db):
    a = a if isinstance(a, list) else pieces_of(a)
    b = b if isinstance(b, list) else pieces_of(b)
    a = jnp.concatenate([a[i] for i in LEFT], da)
    b = jnp.concatenate([b[i] for i in RIGHT], db)
    return lax.dot_general(a, b, (((da,), (db,)), ((), ())), preferred_element_type=F32)


def nn(a, b):
    return product(a, b, 1, 0)


def nt(a, b):
    return product(a, b, 1, 1)


def tn(a, b):
    return product(a, b, 0, 0)


def iota(shape, dim):
    return lax.broadcasted_iota(jnp.int32, shape, dim)


def tri_inverse_128(blocks):
    r = iota((BLK, BLK), 0)
    c = iota((BLK, BLK), 1)
    inv = [jnp.where(r == c, 1.0 / jnp.where(r == c, d, 1.0), 0.0) for d in blocks]
    m = 1
    while m < BLK:
        pick = (r // (2 * m) == c // (2 * m)) & (r // m != c // m) & (r > c)
        low = [jnp.where(pick, d, 0.0) for d in blocks]
        if m == 1:
            mid = [jnp.sum(x, axis=0, keepdims=True) for x in inv]
            row = [jnp.sum(x, axis=1, keepdims=True) for x in inv]
            inv = [x - rr * l * mm for x, l, rr, mm in zip(inv, low, row, mid)]
        else:
            half = [nn(l, x) for l, x in zip(low, inv)]
            inv = [x - nn(x, h) for x, h in zip(inv, half)]
        m *= 2
    return inv


def row(x, s):
    return jnp.broadcast_to(x[s : s + 1, :], (8, BLK))


def col(x, c):
    return jnp.broadcast_to(x[:, c : c + 1], (8, BLK))


def cholesky_rows(blocks, j0):
    tiles = range(STEP // 8)
    shape = (8, BLK)
    r = iota(shape, 0)
    lane = iota(shape, 1)
    here = (lane >= j0) & (lane < j0 + STEP)
    x = [[w[8 * v : 8 * v + 8, :] for v in tiles] for w in blocks]
    part = [lane >= SHARE * i for i in range(len(blocks))]
    c = [[None] * (8 * v + 8) for v in tiles]
    for v in tiles:
        for t in range(8 * v + 8):
            both = col(x[0][v], j0 + t)
            for i in range(1, len(blocks)):
                both = jnp.where(part[i], col(x[i][v], j0 + t), both)
            c[v][t] = both
    mult = []
    roots = [None for _ in tiles]
    for t in range(STEP):
        first, s = divmod(t, 8)
        root = lax.rsqrt(row(c[first][t], s))
        recip = root * root
        m = {v: c[v][t] * recip for v in tiles if v >= first}
        m[first] = jnp.where(r > s, m[first], 0.0)
        for u in range(t + 1, STEP):
            y = row(c[u // 8][t], u % 8)
            for v in range(u // 8, len(tiles)):
                c[v][u] = c[v][u] - m[v] * y
        mult.append(m)
        roots[first] = root if s == 0 else jnp.where(r == s, root, roots[first])
    out = []
    for i, w in enumerate(x):
        rest = [jnp.where(here, jnp.where(lane == r + j0 + 8 * v, 1.0, 0.0), w[v]) for v in tiles]
        for t in range(STEP):
            first, s = divmod(t, 8)
            y = row(rest[first], s)
            for v, m in mult[t].items():
                rest[v] = rest[v] - col(m, SHARE * i) * y
        out.append(jnp.concatenate([rest[v] * col(roots[v], SHARE * i) for v in tiles], 0))
    return out


def chol_inverse_128(src, dst, count):
    c = iota((STEP, BLK), 1)
    steps = BLK // STEP
    w = [[src[i, q * STEP : (q + 1) * STEP, :] for q in range(steps)] for i in range(count)]
    for j in range(steps):
        j0 = j * STEP
        done = cholesky_rows([w[i][j] for i in range(count)], j0)
        for i, x in enumerate(done):
            dst[i, j0 : j0 + STEP, :] = jnp.where(c < j0 + STEP, x, 0.0)
            if j + 1 < steps:
                y = tn(x, x)
                here = (c >= j0) & (c < j0 + STEP)
                for q in range(j + 1, steps):
                    w[i][q] = jnp.where(here, 0.0, w[i][q]) - y[q * STEP : (q + 1) * STEP, :]


def call(kernel, mib, outs, scratch, scalars, *arrays):
    smem = pl.BlockSpec(memory_space=pltpu.SMEM)
    vmem = pl.BlockSpec(memory_space=pltpu.VMEM)
    outs = [s if isinstance(s, jax.ShapeDtypeStruct) else jax.ShapeDtypeStruct(s, F32) for s in outs]
    return pl.pallas_call(
        kernel,
        out_shape=outs,
        in_specs=[smem] + [vmem] * len(arrays),
        out_specs=[vmem] * len(outs),
        scratch_shapes=[pltpu.VMEM(s, F32) for s in scratch],
        compiler_params=pltpu.CompilerParams(vmem_limit_bytes=mib * 1024 * 1024),
    )(scalars, *arrays)


def pack_kernel(pos, f, u, p0, p1, p2, p3, left, u_s):
    depth, group = pos[0], pos[4]
    u_s[...] = u[...].T
    start = pl.multiple_of(group * B, B)
    for shift, out in enumerate((p0, p1, p2, p3)):
        for k in range(4):
            out[k * BLK : (k + 1) * BLK, :] = f[:, pl.ds(start + k * BLK, BLK)]
        first = pl.multiple_of(((depth + shift) % 4) * (K // 4), K // 4)
        out[4 * BLK :, :] = u_s[pl.ds(first, K // 4), :]
    left[...] = f[:, : 2 * B]


def first_kernel(pos, p0, p1, p2, p3, inv_ref, v_ref, g_ref, d_s):
    depth = pos[0]
    for shift, p in enumerate((p0, p1, p2, p3)):
        slot = (depth + 4 - shift) % 4
        d_s[slot] = p[: 4 * BLK, :].reshape(4, BLK, BLK)
        v_ref[slot] = p[4 * BLK :, :]
    diag = tri_inverse_128([d_s[i, i] for i in range(4)])
    low10 = -nn(diag[1], nn(d_s[1, 0], diag[0]))
    low32 = -nn(diag[3], nn(d_s[3, 2], diag[2]))
    zero = jnp.zeros((BLK, BLK), F32)
    top = jnp.concatenate([jnp.concatenate([diag[0], zero], 1), jnp.concatenate([low10, diag[1]], 1)], 0)
    bot = jnp.concatenate([jnp.concatenate([diag[2], zero], 1), jnp.concatenate([low32, diag[3]], 1)], 0)
    below = jnp.concatenate(
        [jnp.concatenate([d_s[i, 0], d_s[i, 1]], 1) for i in (2, 3)], 0
    )
    cross = -nn(bot, nn(below, top))
    inv = jnp.concatenate(
        [
            jnp.concatenate([top, jnp.zeros((2 * BLK, 2 * BLK), F32)], 1),
            jnp.concatenate([cross, bot], 1),
        ],
        0,
    )
    terms = pieces_of(inv)
    for i, x in enumerate(terms):
        inv_ref[i] = x
    v = jnp.concatenate([v_ref[i] for i in range(4)], 1)
    g_ref[...] = jnp.where(pos[3] == 0, nt(v, terms), 0.0)


def left_product(pos, g, left, panel, out):
    terms = pieces_of(g)
    for shift, piece in enumerate(left):
        slot = (pos[0] + 4 - shift) % 4
        out[slot] = nt(terms, piece[:, (panel - 1) * B : panel * B])


def left0_kernel(pos, got1, got2, l0, l1, l2, l3, sum_ref, out):
    g = got1[...] + got2[...]
    sum_ref[...] = g
    left_product(pos, g, (l0, l1, l2, l3), 1, out)


def left1_kernel(pos, g, l0, l1, l2, l3, out):
    left_product(pos, g[...], (l0, l1, l2, l3), 2, out)


def solve(v, t, inv, out):
    for i in range(4):
        out[i] = v[i] - t[i]
    return nt(jnp.concatenate([out[i] for i in range(4)], 1), [inv[i] for i in range(3)])


def second_kernel(pos, v, t, inv, v_ref, g_ref):
    g_ref[...] = jnp.where(pos[3] == 1, solve(v, t, inv, v_ref), 0.0)


def third_kernel(pos, v, t, inv, g0, g1, keep, send, v_s):
    h = K // 8
    g2 = solve(v, t, inv, v_s)
    mine, theirs = slice(0, h), slice(h, 2 * h)
    owns, helps = pos[3] == 2, pos[3] == 10
    for ref, first, second in ((keep, mine, theirs), (send, theirs, mine)):
        for i, g in enumerate((g0, g1)):
            ref[:, i * B : (i + 1) * B] = jnp.where(helps, g[second, :], 0.0)
        ref[:, 2 * B :] = jnp.where(owns, g2[first], 0.0)


def last_kernel(pos, f, u, a0, a1, a2, a3, others, f_ref, u_ref, t_s, h_s, s_s, src, dst):
    depth, core, base = pos[0], pos[1], pos[2]
    for shift, mine in enumerate((a0, a1, a2, a3)):
        slot = (depth + 4 - shift) % 4
        t_s[slot * 2 + core] = mine[...]
        t_s[slot * 2 + 1 - core] = others[shift]
    acc = jnp.where(iota((K, K), 0) == iota((K, K), 1), 1.0, 0.0)
    v = u[...]
    for j in range(NB):
        gt = t_s[:, :, j * K : (j + 1) * K].reshape(K, K)
        acc = acc + nt(gt, gt)
        v = v - nt(f[:, j * K : (j + 1) * K], gt)
        for k in range(2):
            sl = slice(k * BLK, (k + 1) * BLK)
            h_s[j, k, 0:K, :] = acc[:, sl]
            h_s[j, k, K : K + BLK, :] = v[:, sl]
        g = gt.T
        if j == 0:
            first = g
        else:
            for k in range(2):
                h_s[j - 1, k, K + BLK :, :] = g[:, k * BLK : (k + 1) * BLK]

    def before(j):
        if j == 0:
            return u[...]
        return jnp.concatenate([h_s[j - 1, k, K : K + BLK, :] for k in range(2)], 1)

    def step(i, carry):
        del carry

        @pl.when(i == 0)
        def _():
            for j in range(NB):
                src[j] = h_s[j, 0, 0:BLK, :]

        chol_inverse_128(src, dst, NB)

        @pl.when(i == 0)
        def _():
            for j in range(NB):
                low = nt(h_s[j, 0, BLK:, :], dst[j])
                h_s[j, 0, BLK:, :] = low
                low = h_s[j, 1, BLK:, :] - nt(low, low[0:BLK, :])
                h_s[j, 1, BLK:, :] = low
                src[j] = low[0:BLK, :]

        @pl.when(i == 1)
        def _():
            for j in range(NB):
                h_s[j, 1, K:, :] = nt(h_s[j, 1, K:, :], dst[j])
            for j in range(NB):
                if j == 0:
                    g = first
                else:
                    g = jnp.concatenate([h_s[j - 1, k, K + BLK :, :] for k in range(2)], 1)
                full = nt(jnp.concatenate([g, before(j)], 0), g)
                eye = jnp.where(iota((K, K), 0) == iota((K, K), 1), 1.0, 0.0)
                s_s[j, 0:K, :] = full[0:K] + eye
                s_s[j, K:, :] = full[K:] + f[:, j * K : (j + 1) * K]
                src[j] = s_s[j, 0:BLK, 0:BLK]

        @pl.when(i == 2)
        def _():
            for j in range(NB):
                low = nt(s_s[j, BLK:, 0:BLK], dst[j])
                s_s[j, BLK:, 0:BLK] = low
                low = s_s[j, BLK:, BLK:] - nt(low, low[0:BLK, :])
                s_s[j, BLK:, BLK:] = low
                src[j] = low[0:BLK, :]

        @pl.when(i == 3)
        def _():
            rows = base + iota((BLK, BLK), 0)
            cols = iota((BLK, BLK), 1)
            for j in range(NB):
                lo = j * K
                f_ref[:, lo : lo + BLK] = jnp.where(rows >= cols + lo, s_s[j, K:, 0:BLK], 0.0)
                lo = lo + BLK
                new = nt(s_s[j, K:, BLK:], dst[j])
                f_ref[:, lo : lo + BLK] = jnp.where(rows >= cols + lo, new, 0.0)

        return 0

    lax.fori_loop(0, 4, step, 0)
    rows = base + iota((BLK, K), 0)
    out = before(2)
    for p in range(1, PANELS):
        out = jnp.where(rows >= p * B, before(2 * p + 2), out)
    u_ref[...] = out


def last_call(pos, factor, update, *pieces):
    return call(
        last_kernel,
        32,
        [factor.shape, update.shape],
        [
            (8, K // 8, PANELS * B),
            (NB, 2, K + BLK + K, BLK),
            (NB, K + BLK, K),
            (NB, BLK, BLK),
            (NB, BLK, BLK),
        ],
        pos,
        factor,
        update,
        *pieces,
    )


def device(x, y, z, core):
    return (((z // 2) * 2 + core) * 8 + y * 2 + z % 2) * 4 + x


def owner(p, x):
    return p * 4 + x


def helper(p, x):
    return (8 + p) * 4 + x


def helper_ring(shift):
    return [(helper(p, x), helper(p, (x + shift) % 4)) for p in (1, 2) for x in range(4)]


def move(value, pairs):
    return lax.ppermute(value, AXES, pairs)


def depth_ring(shift):
    return [(owner(p, x), owner(p, (x + shift) % 4)) for p in range(PANELS) for x in range(4)]


def tree_steps():
    y0, z0 = 1, 0
    plans = (
        (("y", 2), ("y", 1), ("z", 4), ("z", 2), ("z", 1)),
        (("z", 4), ("z", 2), ("z", 1), ("y", 2), ("y", 1)),
    )
    held = [[(0, 0)], [(0, 0)]]
    for i in range(5):
        pairs = []
        for core in range(2):
            axis, hop = plans[core][i]
            new = []
            for dy, dz in held[core]:
                to = (dy + hop, dz) if axis == "y" else (dy, dz + hop)
                new.append(to)
                for x in range(4):
                    pairs.append(
                        (
                            device(x, (y0 + dy) % 4, (z0 + dz) % 8, core),
                            device(x, (y0 + to[0]) % 4, (z0 + to[1]) % 8, core),
                        )
                    )
            held[core] += new
        yield pairs


def everywhere(shift):
    return [((i // 4) * 4 + i % 4, (i // 4) * 4 + (i % 4 + shift) % 4) for i in range(256)]


def partner():
    return [
        (device(x, y, z, c), device(x, y, z, 1 - c))
        for x in range(4)
        for y in range(4)
        for z in range(8)
        for c in range(2)
    ]


def on_device(factor, update):
    core = lax.axis_index("row") % 2
    depth = lax.axis_index("depth")
    flat = lax.axis_index(AXES)
    pos = jnp.stack([depth, core, flat * BLK, flat // 4, jnp.minimum(flat // 4, PANELS - 1)])
    pos = pos.astype(jnp.int32)
    quarter, half = K // 4, K // 8

    packed = (4 * BLK + quarter, BLK)
    p0, p1, p2, p3, left = call(
        pack_kernel, 8, [packed] * 4 + [(BLK, 2 * B)], [(K, BLK)], pos, factor, update
    )
    left = move(left, [(owner(p, x), helper(p, x)) for p in (1, 2) for x in range(4)])
    parts = [p0] + [move(p, depth_ring(s)) for s, p in ((1, p1), (2, p2), (3, p3))]
    lefts = [left] + [move(left, helper_ring(s)) for s in range(1, 4)]
    inv, v, g0 = call(
        first_kernel,
        16,
        [jax.ShapeDtypeStruct((3, B, B), jnp.bfloat16), (4, quarter, BLK), (quarter, B)],
        [(4, 4, BLK, BLK)],
        pos,
        *parts,
    )
    got1 = move(g0, [(owner(0, x), helper(1, x)) for x in range(4)])
    g0, got1 = lax.optimization_barrier((g0, got1))
    got2 = move(g0, [(owner(0, x), helper(2, x)) for x in range(4)])
    g0, t = call(
        left0_kernel, 16, [(quarter, B), (4, quarter, BLK)], [], pos, got1, got2, *lefts
    )
    t = move(t, [(helper(p, x), owner(p, x)) for p in (1, 2) for x in range(4)])
    v, g1 = call(second_kernel, 16, [(4, quarter, BLK), (quarter, B)], [], pos, v, t, inv)
    g1 = move(g1, [(owner(1, x), helper(2, x)) for x in range(4)])
    (t,) = call(left1_kernel, 16, [(4, quarter, BLK)], [], pos, g1, *lefts)
    t = move(t, [(helper(2, x), owner(2, x)) for x in range(4)])
    keep, send = call(
        third_kernel, 16, [(half, PANELS * B)] * 2, [(4, quarter, BLK)], pos, v, t, inv, g0, g1
    )
    swap = [(owner(2, x), helper(2, x)) for x in range(4)]
    value = keep + move(send, swap + [(b, a) for a, b in swap])
    for pairs in tree_steps():
        value = value + move(value, pairs)
    mine = [value] + [move(value, everywhere(s)) for s in range(1, 4)]
    others = move(jnp.stack(mine), partner())
    return tuple(last_call(pos, factor, update, *mine, others))


def solution(mesh):
    spec = P(AXES, None)
    return jax.shard_map(
        on_device, mesh=mesh, in_specs=(spec, spec), out_specs=(spec, spec), check_vma=False
    )
```

```python
import jax
import jax.numpy as jnp
from jax import lax
from jax.experimental import pallas as pl
from jax.experimental.pallas import tpu as pltpu
from jax.sharding import PartitionSpec as P


B = 512
K = 256
PANELS = 3
BLK = 128
STEP = 16
NB = 6
AXES = ("row", "col", "depth")
PASSES = 6
SHARE = 16
F32 = jnp.float32


def pieces_of(x):
    terms = []
    for _ in range(2 if PASSES == 3 else 3):
        terms.append(x.astype(jnp.bfloat16))
        x = x - terms[-1].astype(F32)
    return terms


LEFT, RIGHT = ((0, 0, 1), (0, 1, 0)) if PASSES == 3 else ((0, 0, 0, 1, 1, 2), (0, 1, 2, 0, 1, 0))


def product(a, b, da, db):
    a = a if isinstance(a, list) else pieces_of(a)
    b = b if isinstance(b, list) else pieces_of(b)
    a = jnp.concatenate([a[i] for i in LEFT], da)
    b = jnp.concatenate([b[i] for i in RIGHT], db)
    return lax.dot_general(a, b, (((da,), (db,)), ((), ())), preferred_element_type=F32)


def nn(a, b):
    return product(a, b, 1, 0)


def nt(a, b):
    return product(a, b, 1, 1)


def tn(a, b):
    return product(a, b, 0, 0)


def iota(shape, dim):
    return lax.broadcasted_iota(jnp.int32, shape, dim)


def tri_inverse_128(blocks):
    r = iota((BLK, BLK), 0)
    c = iota((BLK, BLK), 1)
    inv = [jnp.where(r == c, 1.0 / jnp.where(r == c, d, 1.0), 0.0) for d in blocks]
    m = 1
    while m < BLK:
        pick = (r // (2 * m) == c // (2 * m)) & (r // m != c // m) & (r > c)
        low = [jnp.where(pick, d, 0.0) for d in blocks]
        if m == 1:
            mid = [jnp.sum(x, axis=0, keepdims=True) for x in inv]
            row = [jnp.sum(x, axis=1, keepdims=True) for x in inv]
            inv = [x - rr * l * mm for x, l, rr, mm in zip(inv, low, row, mid)]
        else:
            half = [nn(l, x) for l, x in zip(low, inv)]
            inv = [x - nn(x, h) for x, h in zip(inv, half)]
        m *= 2
    return inv


def row(x, s):
    return jnp.broadcast_to(x[s : s + 1, :], (8, BLK))


def col(x, c):
    return jnp.broadcast_to(x[:, c : c + 1], (8, BLK))


def cholesky_rows(blocks, j0):
    tiles = range(STEP // 8)
    shape = (8, BLK)
    r = iota(shape, 0)
    lane = iota(shape, 1)
    here = (lane >= j0) & (lane < j0 + STEP)
    x = [[w[8 * v : 8 * v + 8, :] for v in tiles] for w in blocks]
    part = [lane >= SHARE * i for i in range(len(blocks))]
    c = [[None] * (8 * v + 8) for v in tiles]
    for v in tiles:
        for t in range(8 * v + 8):
            both = col(x[0][v], j0 + t)
            for i in range(1, len(blocks)):
                both = jnp.where(part[i], col(x[i][v], j0 + t), both)
            c[v][t] = both
    mult = []
    roots = [None for _ in tiles]
    for t in range(STEP):
        first, s = divmod(t, 8)
        root = lax.rsqrt(row(c[first][t], s))
        recip = root * root
        m = {v: c[v][t] * recip for v in tiles if v >= first}
        m[first] = jnp.where(r > s, m[first], 0.0)
        for u in range(t + 1, STEP):
            y = row(c[u // 8][t], u % 8)
            for v in range(u // 8, len(tiles)):
                c[v][u] = c[v][u] - m[v] * y
        mult.append(m)
        roots[first] = root if s == 0 else jnp.where(r == s, root, roots[first])
    out = []
    for i, w in enumerate(x):
        rest = [jnp.where(here, jnp.where(lane == r + j0 + 8 * v, 1.0, 0.0), w[v]) for v in tiles]
        for t in range(STEP):
            first, s = divmod(t, 8)
            y = row(rest[first], s)
            for v, m in mult[t].items():
                rest[v] = rest[v] - col(m, SHARE * i) * y
        out.append(jnp.concatenate([rest[v] * col(roots[v], SHARE * i) for v in tiles], 0))
    return out


def chol_inverse_128(src, dst, count):
    c = iota((STEP, BLK), 1)
    steps = BLK // STEP
    w = [[src[i, q * STEP : (q + 1) * STEP, :] for q in range(steps)] for i in range(count)]
    for j in range(steps):
        j0 = j * STEP
        done = cholesky_rows([w[i][j] for i in range(count)], j0)
        for i, x in enumerate(done):
            dst[i, j0 : j0 + STEP, :] = jnp.where(c < j0 + STEP, x, 0.0)
            if j + 1 < steps:
                y = tn(x, x)
                here = (c >= j0) & (c < j0 + STEP)
                for q in range(j + 1, steps):
                    w[i][q] = jnp.where(here, 0.0, w[i][q]) - y[q * STEP : (q + 1) * STEP, :]


def call(kernel, mib, outs, scratch, scalars, *arrays):
    smem = pl.BlockSpec(memory_space=pltpu.SMEM)
    vmem = pl.BlockSpec(memory_space=pltpu.VMEM)
    outs = [s if isinstance(s, jax.ShapeDtypeStruct) else jax.ShapeDtypeStruct(s, F32) for s in outs]
    return pl.pallas_call(
        kernel,
        out_shape=outs,
        in_specs=[smem] + [vmem] * len(arrays),
        out_specs=[vmem] * len(outs),
        scratch_shapes=[pltpu.VMEM(s, F32) for s in scratch],
        compiler_params=pltpu.CompilerParams(vmem_limit_bytes=mib * 1024 * 1024),
    )(scalars, *arrays)


def pack_kernel(pos, f, u, p0, p1, p2, p3, left_a, left_b, u_s):
    depth, group = pos[0], pos[4]
    u_s[...] = u[...].T
    start = pl.multiple_of(group * B, B)
    for shift, out in enumerate((p0, p1, p2, p3)):
        for k in range(4):
            out[k * BLK : (k + 1) * BLK, :] = f[:, pl.ds(start + k * BLK, BLK)]
        first = pl.multiple_of(((depth + shift) % 4) * (K // 4), K // 4)
        out[4 * BLK :, :] = u_s[pl.ds(first, K // 4), :]
    left_a[...] = f[:, :B]
    left_b[...] = f[:, B : 2 * B]


def first_kernel(pos, p0, p1, p2, p3, inv_ref, v_ref, g_ref, d_s):
    depth = pos[0]
    for shift, p in enumerate((p0, p1, p2, p3)):
        slot = (depth + 4 - shift) % 4
        d_s[slot] = p[: 4 * BLK, :].reshape(4, BLK, BLK)
        v_ref[slot] = p[4 * BLK :, :]
    diag = tri_inverse_128([d_s[i, i] for i in range(4)])
    low10 = -nn(diag[1], nn(d_s[1, 0], diag[0]))
    low32 = -nn(diag[3], nn(d_s[3, 2], diag[2]))
    zero = jnp.zeros((BLK, BLK), F32)
    top = jnp.concatenate([jnp.concatenate([diag[0], zero], 1), jnp.concatenate([low10, diag[1]], 1)], 0)
    bot = jnp.concatenate([jnp.concatenate([diag[2], zero], 1), jnp.concatenate([low32, diag[3]], 1)], 0)
    below = jnp.concatenate(
        [jnp.concatenate([d_s[i, 0], d_s[i, 1]], 1) for i in (2, 3)], 0
    )
    cross = -nn(bot, nn(below, top))
    inv = jnp.concatenate(
        [
            jnp.concatenate([top, jnp.zeros((2 * BLK, 2 * BLK), F32)], 1),
            jnp.concatenate([cross, bot], 1),
        ],
        0,
    )
    terms = pieces_of(inv)
    for i, x in enumerate(terms):
        inv_ref[i] = x
    v = jnp.concatenate([v_ref[i] for i in range(4)], 1)
    g_ref[...] = jnp.where(pos[3] == 0, nt(v, terms), 0.0)


def left_product(pos, g, left, out):
    terms = pieces_of(g)
    for shift, piece in enumerate(left):
        slot = (pos[0] + 4 - shift) % 4
        out[slot] = nt(terms, piece[...])


def left0_kernel(pos, got1, got2, l0, l1, l2, l3, sum_ref, out):
    g = got1[...] + got2[...]
    sum_ref[...] = g
    left_product(pos, g, (l0, l1, l2, l3), out)


def left1_kernel(pos, g, l0, l1, l2, l3, out):
    left_product(pos, g[...], (l0, l1, l2, l3), out)


def solve(v, t, inv, out):
    for i in range(4):
        out[i] = v[i] - t[i]
    return nt(jnp.concatenate([out[i] for i in range(4)], 1), [inv[i] for i in range(3)])


def second_kernel(pos, v, t, inv, v_ref, g_ref):
    g_ref[...] = jnp.where(pos[3] == 1, solve(v, t, inv, v_ref), 0.0)


def third_kernel(pos, v, t, inv, g0, g1, keep, send, v_s):
    h = K // 8
    g2 = solve(v, t, inv, v_s)
    mine, theirs = slice(0, h), slice(h, 2 * h)
    owns, helps = pos[3] == 2, pos[3] == 10
    for ref, first, second in ((keep, mine, theirs), (send, theirs, mine)):
        for i, g in enumerate((g0, g1)):
            ref[:, i * B : (i + 1) * B] = jnp.where(helps, g[second, :], 0.0)
        ref[:, 2 * B :] = jnp.where(owns, g2[first], 0.0)


def last_kernel(pos, f, u, a0, a1, a2, a3, others, f_ref, u_ref, t_s, h_s, s_s, src, dst):
    depth, core, base = pos[0], pos[1], pos[2]
    for shift, mine in enumerate((a0, a1, a2, a3)):
        slot = (depth + 4 - shift) % 4
        t_s[slot * 2 + core] = mine[...]
        t_s[slot * 2 + 1 - core] = others[shift]
    acc = jnp.where(iota((K, K), 0) == iota((K, K), 1), 1.0, 0.0)
    v = u[...]
    for j in range(NB):
        gt = t_s[:, :, j * K : (j + 1) * K].reshape(K, K)
        acc = acc + nt(gt, gt)
        v = v - nt(f[:, j * K : (j + 1) * K], gt)
        for k in range(2):
            sl = slice(k * BLK, (k + 1) * BLK)
            h_s[j, k, 0:K, :] = acc[:, sl]
            h_s[j, k, K : K + BLK, :] = v[:, sl]
        g = gt.T
        if j == 0:
            first = g
        else:
            for k in range(2):
                h_s[j - 1, k, K + BLK :, :] = g[:, k * BLK : (k + 1) * BLK]

    def before(j):
        if j == 0:
            return u[...]
        return jnp.concatenate([h_s[j - 1, k, K : K + BLK, :] for k in range(2)], 1)

    def step(i, carry):
        del carry

        @pl.when(i == 0)
        def _():
            for j in range(NB):
                src[j] = h_s[j, 0, 0:BLK, :]

        chol_inverse_128(src, dst, NB)

        @pl.when(i == 0)
        def _():
            for j in range(NB):
                low = nt(h_s[j, 0, BLK:, :], dst[j])
                h_s[j, 0, BLK:, :] = low
                low = h_s[j, 1, BLK:, :] - nt(low, low[0:BLK, :])
                h_s[j, 1, BLK:, :] = low
                src[j] = low[0:BLK, :]

        @pl.when(i == 1)
        def _():
            for j in range(NB):
                h_s[j, 1, K:, :] = nt(h_s[j, 1, K:, :], dst[j])
            for j in range(NB):
                if j == 0:
                    g = first
                else:
                    g = jnp.concatenate([h_s[j - 1, k, K + BLK :, :] for k in range(2)], 1)
                full = nt(jnp.concatenate([g, before(j)], 0), g)
                eye = jnp.where(iota((K, K), 0) == iota((K, K), 1), 1.0, 0.0)
                s_s[j, 0:K, :] = full[0:K] + eye
                s_s[j, K:, :] = full[K:] + f[:, j * K : (j + 1) * K]
                src[j] = s_s[j, 0:BLK, 0:BLK]

        @pl.when(i == 2)
        def _():
            for j in range(NB):
                low = nt(s_s[j, BLK:, 0:BLK], dst[j])
                s_s[j, BLK:, 0:BLK] = low
                low = s_s[j, BLK:, BLK:] - nt(low, low[0:BLK, :])
                s_s[j, BLK:, BLK:] = low
                src[j] = low[0:BLK, :]

        @pl.when(i == 3)
        def _():
            rows = base + iota((BLK, BLK), 0)
            cols = iota((BLK, BLK), 1)
            for j in range(NB):
                lo = j * K
                f_ref[:, lo : lo + BLK] = jnp.where(rows >= cols + lo, s_s[j, K:, 0:BLK], 0.0)
                lo = lo + BLK
                new = nt(s_s[j, K:, BLK:], dst[j])
                f_ref[:, lo : lo + BLK] = jnp.where(rows >= cols + lo, new, 0.0)

        return 0

    lax.fori_loop(0, 4, step, 0)
    rows = base + iota((BLK, K), 0)
    out = before(2)
    for p in range(1, PANELS):
        out = jnp.where(rows >= p * B, before(2 * p + 2), out)
    u_ref[...] = out


def last_call(pos, factor, update, *pieces):
    return call(
        last_kernel,
        32,
        [factor.shape, update.shape],
        [
            (8, K // 8, PANELS * B),
            (NB, 2, K + BLK + K, BLK),
            (NB, K + BLK, K),
            (NB, BLK, BLK),
            (NB, BLK, BLK),
        ],
        pos,
        factor,
        update,
        *pieces,
    )


def device(x, y, z, core):
    return (((z // 2) * 2 + core) * 8 + y * 2 + z % 2) * 4 + x


def owner(p, x):
    return p * 4 + x


def helper(p, x):
    return (8 + p) * 4 + x


def helper_ring(shift):
    return [(helper(p, x), helper(p, (x + shift) % 4)) for p in (1, 2) for x in range(4)]


def move(value, pairs):
    return lax.ppermute(value, AXES, pairs)


def depth_ring(shift):
    return [(owner(p, x), owner(p, (x + shift) % 4)) for p in range(PANELS) for x in range(4)]


def spread_steps():
    y0, z0 = 1, 0
    y = [("y", 2), ("y", 1), ("y", 3)]
    z = [("z", 4), ("z", 2), ("z", 6)]
    plans = ((y, z, [("z", 1)]), (z, [("z", 1)], y))
    held = [[(0, 0)], [(0, 0)]]
    for stage in range(3):
        moves = []
        new = [[], []]
        for i in range(3):
            pairs = []
            for core in range(2):
                if i >= len(plans[core][stage]):
                    continue
                axis, hop = plans[core][stage][i]
                for dy, dz in held[core]:
                    to = (dy + hop, dz) if axis == "y" else (dy, dz + hop)
                    new[core].append(to)
                    for x in range(4):
                        pairs.append(
                            (
                                device(x, (y0 + dy) % 4, (z0 + dz) % 8, core),
                                device(x, (y0 + to[0]) % 4, (z0 + to[1]) % 8, core),
                            )
                        )
            moves.append(pairs)
        for core in range(2):
            held[core] += new[core]
        yield moves


def everywhere(shift):
    return [((i // 4) * 4 + i % 4, (i // 4) * 4 + (i % 4 + shift) % 4) for i in range(256)]


def partner():
    return [
        (device(x, y, z, c), device(x, y, z, 1 - c))
        for x in range(4)
        for y in range(4)
        for z in range(8)
        for c in range(2)
    ]


def steps(factor, update):
    core = lax.axis_index("row") % 2
    depth = lax.axis_index("depth")
    flat = lax.axis_index(AXES)
    pos = jnp.stack([depth, core, flat * BLK, flat // 4, jnp.minimum(flat // 4, PANELS - 1)])
    pos = pos.astype(jnp.int32)
    quarter, half = K // 4, K // 8

    packed = (4 * BLK + quarter, BLK)
    p0, p1, p2, p3, left_a, left_b = call(
        pack_kernel, 8, [packed] * 4 + [(BLK, B)] * 2, [(K, BLK)], pos, factor, update
    )
    left_a = move(left_a, [(owner(p, x), helper(p, x)) for p in (1, 2) for x in range(4)])
    left_b = move(left_b, [(owner(2, x), helper(2, x)) for x in range(4)])
    parts, lefts = [p0], [left_a]
    for s, p in ((1, p1), (2, p2), (3, p3)):
        parts.append(move(p, depth_ring(s)))
    for s in range(1, 4):
        lefts.append(move(left_a, helper_ring(s)))
    rights = [left_b]
    for s in range(1, 4):
        rights.append(move(left_b, helper_ring(s)[4:]))
    inv, v, g0 = call(
        first_kernel,
        16,
        [jax.ShapeDtypeStruct((3, B, B), jnp.bfloat16), (4, quarter, BLK), (quarter, B)],
        [(4, 4, BLK, BLK)],
        pos,
        *parts,
    )
    got1 = move(g0, [(owner(0, x), helper(1, x)) for x in range(4)])
    g0, got1 = lax.optimization_barrier((g0, got1))
    got2 = move(g0, [(owner(0, x), helper(2, x)) for x in range(4)])
    g0, t = call(
        left0_kernel, 16, [(quarter, B), (4, quarter, BLK)], [], pos, got1, got2, *lefts
    )
    t = move(t, [(helper(p, x), owner(p, x)) for p in (1, 2) for x in range(4)])
    v, g1 = call(second_kernel, 16, [(4, quarter, BLK), (quarter, B)], [], pos, v, t, inv)
    g1 = move(g1, [(owner(1, x), helper(2, x)) for x in range(4)])
    (t,) = call(left1_kernel, 16, [(4, quarter, BLK)], [], pos, g1, *rights)
    t = move(t, [(helper(2, x), owner(2, x)) for x in range(4)])
    keep, send = call(
        third_kernel, 16, [(half, PANELS * B)] * 2, [(4, quarter, BLK)], pos, v, t, inv, g0, g1
    )
    swap = [(owner(2, x), helper(2, x)) for x in range(4)]
    value = keep + move(send, swap + [(b, a) for a, b in swap])
    for moves in spread_steps():
        value = sum([move(value, pairs) for pairs in moves], value)
    mine = [value] + [move(value, everywhere(s)) for s in range(1, 4)]
    others = move(jnp.stack(mine), partner())
    return tuple(last_call(pos, factor, update, *mine, others))


def solution(mesh):
    spec = P(AXES, None)
    return jax.shard_map(
        steps, mesh=mesh, in_specs=(spec, spec), out_specs=(spec, spec), check_vma=False
    )
```

```python
import jax
import jax.numpy as jnp
from jax import lax
from jax.experimental import pallas as pl
from jax.experimental.pallas import tpu as pltpu
from jax.sharding import PartitionSpec as P


B = 512
K = 256
PANELS = 3
BLK = 128
STEP = 16
NB = 6
AXES = ("row", "col", "depth")
PASSES = 6
SHARE = 16
F32 = jnp.float32


def pieces_of(x):
    terms = []
    for _ in range(2 if PASSES == 3 else 3):
        terms.append(x.astype(jnp.bfloat16))
        x = x - terms[-1].astype(F32)
    return terms


LEFT, RIGHT = ((0, 0, 1), (0, 1, 0)) if PASSES == 3 else ((0, 0, 0, 1, 1, 2), (0, 1, 2, 0, 1, 0))


def product(a, b, da, db):
    a = a if isinstance(a, list) else pieces_of(a)
    b = b if isinstance(b, list) else pieces_of(b)
    a = jnp.concatenate([a[i] for i in LEFT], da)
    b = jnp.concatenate([b[i] for i in RIGHT], db)
    return lax.dot_general(a, b, (((da,), (db,)), ((), ())), preferred_element_type=F32)


def nn(a, b):
    return product(a, b, 1, 0)


def nt(a, b):
    return product(a, b, 1, 1)


def tn(a, b):
    return product(a, b, 0, 0)


def iota(shape, dim):
    return lax.broadcasted_iota(jnp.int32, shape, dim)


def tri_inverse_128(blocks):
    r = iota((BLK, BLK), 0)
    c = iota((BLK, BLK), 1)
    inv = [jnp.where(r == c, 1.0 / jnp.where(r == c, d, 1.0), 0.0) for d in blocks]
    m = 1
    while m < BLK:
        pick = (r // (2 * m) == c // (2 * m)) & (r // m != c // m) & (r > c)
        low = [jnp.where(pick, d, 0.0) for d in blocks]
        if m == 1:
            mid = [jnp.sum(x, axis=0, keepdims=True) for x in inv]
            row = [jnp.sum(x, axis=1, keepdims=True) for x in inv]
            inv = [x - rr * l * mm for x, l, rr, mm in zip(inv, low, row, mid)]
        else:
            half = [nn(l, x) for l, x in zip(low, inv)]
            inv = [x - nn(x, h) for x, h in zip(inv, half)]
        m *= 2
    return inv


def row(x, s):
    return jnp.broadcast_to(x[s : s + 1, :], (8, BLK))


def col(x, c):
    return jnp.broadcast_to(x[:, c : c + 1], (8, BLK))


def cholesky_rows(blocks, j0):
    tiles = range(STEP // 8)
    shape = (8, BLK)
    r = iota(shape, 0)
    lane = iota(shape, 1)
    here = (lane >= j0) & (lane < j0 + STEP)
    x = [[w[8 * v : 8 * v + 8, :] for v in tiles] for w in blocks]
    part = [lane >= SHARE * i for i in range(len(blocks))]
    c = [[None] * (8 * v + 8) for v in tiles]
    for v in tiles:
        for t in range(8 * v + 8):
            both = col(x[0][v], j0 + t)
            for i in range(1, len(blocks)):
                both = jnp.where(part[i], col(x[i][v], j0 + t), both)
            c[v][t] = both
    mult = []
    roots = [None for _ in tiles]
    for t in range(STEP):
        first, s = divmod(t, 8)
        root = lax.rsqrt(row(c[first][t], s))
        recip = root * root
        m = {v: c[v][t] * recip for v in tiles if v >= first}
        m[first] = jnp.where(r > s, m[first], 0.0)
        for u in range(t + 1, STEP):
            y = row(c[u // 8][t], u % 8)
            for v in range(u // 8, len(tiles)):
                c[v][u] = c[v][u] - m[v] * y
        mult.append(m)
        roots[first] = root if s == 0 else jnp.where(r == s, root, roots[first])
    out = []
    for i, w in enumerate(x):
        rest = [jnp.where(here, jnp.where(lane == r + j0 + 8 * v, 1.0, 0.0), w[v]) for v in tiles]
        for t in range(STEP):
            first, s = divmod(t, 8)
            y = row(rest[first], s)
            for v, m in mult[t].items():
                rest[v] = rest[v] - col(m, SHARE * i) * y
        out.append(jnp.concatenate([rest[v] * col(roots[v], SHARE * i) for v in tiles], 0))
    return out


def chol_inverse_128(src, dst, count):
    c = iota((STEP, BLK), 1)
    steps = BLK // STEP
    w = [[src[i, q * STEP : (q + 1) * STEP, :] for q in range(steps)] for i in range(count)]
    for j in range(steps):
        j0 = j * STEP
        done = cholesky_rows([w[i][j] for i in range(count)], j0)
        for i, x in enumerate(done):
            dst[i, j0 : j0 + STEP, :] = jnp.where(c < j0 + STEP, x, 0.0)
            if j + 1 < steps:
                y = tn(x, x)
                here = (c >= j0) & (c < j0 + STEP)
                for q in range(j + 1, steps):
                    w[i][q] = jnp.where(here, 0.0, w[i][q]) - y[q * STEP : (q + 1) * STEP, :]


def call(kernel, mib, outs, scratch, scalars, *arrays):
    smem = pl.BlockSpec(memory_space=pltpu.SMEM)
    vmem = pl.BlockSpec(memory_space=pltpu.VMEM)
    outs = [s if isinstance(s, jax.ShapeDtypeStruct) else jax.ShapeDtypeStruct(s, F32) for s in outs]
    return pl.pallas_call(
        kernel,
        out_shape=outs,
        in_specs=[smem] + [vmem] * len(arrays),
        out_specs=[vmem] * len(outs),
        scratch_shapes=[pltpu.VMEM(s, F32) for s in scratch],
        compiler_params=pltpu.CompilerParams(vmem_limit_bytes=mib * 1024 * 1024),
    )(scalars, *arrays)


def pack_kernel(pos, f, u, p0, p1, p2, p3, left_a, left_b, u_s):
    depth, group = pos[0], pos[4]
    u_s[...] = u[...].T
    start = pl.multiple_of(group * B, B)
    for shift, out in enumerate((p0, p1, p2, p3)):
        for k in range(4):
            out[k * BLK : (k + 1) * BLK, :] = f[:, pl.ds(start + k * BLK, BLK)]
        first = pl.multiple_of(((depth + shift) % 4) * (K // 4), K // 4)
        out[4 * BLK :, :] = u_s[pl.ds(first, K // 4), :]
    left_a[...] = f[:, :B]
    left_b[...] = f[:, B : 2 * B]


def first_kernel(pos, p0, p1, p2, p3, inv_ref, v_ref, g_ref, d_s):
    @pl.when(pos[3] < PANELS)
    def _():
        depth = pos[0]
        for shift, p in enumerate((p0, p1, p2, p3)):
            slot = (depth + 4 - shift) % 4
            d_s[slot] = p[: 4 * BLK, :].reshape(4, BLK, BLK)
            v_ref[slot] = p[4 * BLK :, :]
        diag = tri_inverse_128([d_s[i, i] for i in range(4)])
        low10 = -nn(diag[1], nn(d_s[1, 0], diag[0]))
        low32 = -nn(diag[3], nn(d_s[3, 2], diag[2]))
        zero = jnp.zeros((BLK, BLK), F32)
        top = jnp.concatenate([jnp.concatenate([diag[0], zero], 1), jnp.concatenate([low10, diag[1]], 1)], 0)
        bot = jnp.concatenate([jnp.concatenate([diag[2], zero], 1), jnp.concatenate([low32, diag[3]], 1)], 0)
        below = jnp.concatenate(
            [jnp.concatenate([d_s[i, 0], d_s[i, 1]], 1) for i in (2, 3)], 0
        )
        cross = -nn(bot, nn(below, top))
        inv = jnp.concatenate(
            [
                jnp.concatenate([top, jnp.zeros((2 * BLK, 2 * BLK), F32)], 1),
                jnp.concatenate([cross, bot], 1),
            ],
            0,
        )
        terms = pieces_of(inv)
        for i, x in enumerate(terms):
            inv_ref[i] = x
        v = jnp.concatenate([v_ref[i] for i in range(4)], 1)
        g_ref[...] = nt(v, terms)


def left_product(pos, g, left, out):
    terms = pieces_of(g)
    for shift, piece in enumerate(left):
        slot = (pos[0] + 4 - shift) % 4
        out[slot] = nt(terms, piece[...])


def left0_kernel(pos, got1, got2, l0, l1, l2, l3, sum_ref, out):
    @pl.when((pos[3] == 9) | (pos[3] == 10))
    def _():
        g = got1[...] + got2[...]
        sum_ref[...] = g
        left_product(pos, g, (l0, l1, l2, l3), out)


def left1_kernel(pos, g, l0, l1, l2, l3, out):
    @pl.when(pos[3] == 10)
    def _():
        left_product(pos, g[...], (l0, l1, l2, l3), out)


def solve(v, t, inv, out):
    for i in range(4):
        out[i] = v[i] - t[i]
    return nt(jnp.concatenate([out[i] for i in range(4)], 1), [inv[i] for i in range(3)])


def second_kernel(pos, v, t, inv, v_ref, g_ref):
    @pl.when((pos[3] == 1) | (pos[3] == 2))
    def _():
        g_ref[...] = solve(v, t, inv, v_ref)


def third_kernel(pos, v, t, inv, g0, g1, keep, send, v_s):
    h = K // 8
    mine, theirs = slice(0, h), slice(h, 2 * h)
    owns, helps = pos[3] == 2, pos[3] == 10
    for ref in (keep, send):
        ref[...] = jnp.zeros((h, PANELS * B), F32)

    @pl.when(helps)
    def _():
        for ref, rows in ((keep, theirs), (send, mine)):
            for i, g in enumerate((g0, g1)):
                ref[:, i * B : (i + 1) * B] = g[rows, :]

    @pl.when(owns)
    def _():
        g2 = solve(v, t, inv, v_s)
        keep[:, 2 * B :] = g2[mine]
        send[:, 2 * B :] = g2[theirs]


def last_kernel(pos, f, u, a0, a1, a2, a3, others, f_ref, u_ref, t_s, h_s, s_s, src, dst):
    depth, core, base = pos[0], pos[1], pos[2]
    for shift, mine in enumerate((a0, a1, a2, a3)):
        slot = (depth + 4 - shift) % 4
        t_s[slot * 2 + core] = mine[...]
        t_s[slot * 2 + 1 - core] = others[shift]
    acc = jnp.where(iota((K, K), 0) == iota((K, K), 1), 1.0, 0.0)
    v = u[...]
    for j in range(NB):
        gt = t_s[:, :, j * K : (j + 1) * K].reshape(K, K)
        acc = acc + nt(gt, gt)
        v = v - nt(f[:, j * K : (j + 1) * K], gt)
        for k in range(2):
            sl = slice(k * BLK, (k + 1) * BLK)
            h_s[j, k, 0:K, :] = acc[:, sl]
            h_s[j, k, K : K + BLK, :] = v[:, sl]
        g = gt.T
        if j == 0:
            first = g
        else:
            for k in range(2):
                h_s[j - 1, k, K + BLK :, :] = g[:, k * BLK : (k + 1) * BLK]

    def before(j):
        if j == 0:
            return u[...]
        return jnp.concatenate([h_s[j - 1, k, K : K + BLK, :] for k in range(2)], 1)

    def step(i, carry):
        del carry

        @pl.when(i == 0)
        def _():
            for j in range(NB):
                src[j] = h_s[j, 0, 0:BLK, :]

        chol_inverse_128(src, dst, NB)

        @pl.when(i == 0)
        def _():
            for j in range(NB):
                low = nt(h_s[j, 0, BLK:, :], dst[j])
                h_s[j, 0, BLK:, :] = low
                low = h_s[j, 1, BLK:, :] - nt(low, low[0:BLK, :])
                h_s[j, 1, BLK:, :] = low
                src[j] = low[0:BLK, :]

        @pl.when(i == 1)
        def _():
            for j in range(NB):
                h_s[j, 1, K:, :] = nt(h_s[j, 1, K:, :], dst[j])
            for j in range(NB):
                if j == 0:
                    g = first
                else:
                    g = jnp.concatenate([h_s[j - 1, k, K + BLK :, :] for k in range(2)], 1)
                full = nt(jnp.concatenate([g, before(j)], 0), g)
                eye = jnp.where(iota((K, K), 0) == iota((K, K), 1), 1.0, 0.0)
                s_s[j, 0:K, :] = full[0:K] + eye
                s_s[j, K:, :] = full[K:] + f[:, j * K : (j + 1) * K]
                src[j] = s_s[j, 0:BLK, 0:BLK]

        @pl.when(i == 2)
        def _():
            for j in range(NB):
                low = nt(s_s[j, BLK:, 0:BLK], dst[j])
                s_s[j, BLK:, 0:BLK] = low
                low = s_s[j, BLK:, BLK:] - nt(low, low[0:BLK, :])
                s_s[j, BLK:, BLK:] = low
                src[j] = low[0:BLK, :]

        @pl.when(i == 3)
        def _():
            rows = base + iota((BLK, BLK), 0)
            cols = iota((BLK, BLK), 1)
            for j in range(NB):
                lo = j * K
                f_ref[:, lo : lo + BLK] = jnp.where(rows >= cols + lo, s_s[j, K:, 0:BLK], 0.0)
                lo = lo + BLK
                new = nt(s_s[j, K:, BLK:], dst[j])
                f_ref[:, lo : lo + BLK] = jnp.where(rows >= cols + lo, new, 0.0)

        return 0

    lax.fori_loop(0, 4, step, 0)
    rows = base + iota((BLK, K), 0)
    out = before(2)
    for p in range(1, PANELS):
        out = jnp.where(rows >= p * B, before(2 * p + 2), out)
    u_ref[...] = out


def last_call(pos, factor, update, *pieces):
    return call(
        last_kernel,
        32,
        [factor.shape, update.shape],
        [
            (8, K // 8, PANELS * B),
            (NB, 2, K + BLK + K, BLK),
            (NB, K + BLK, K),
            (NB, BLK, BLK),
            (NB, BLK, BLK),
        ],
        pos,
        factor,
        update,
        *pieces,
    )


def device(x, y, z, core):
    return (((z // 2) * 2 + core) * 8 + y * 2 + z % 2) * 4 + x


def owner(p, x):
    return p * 4 + x


def helper(p, x):
    return (8 + p) * 4 + x


def helper_ring(shift):
    return [(helper(p, x), helper(p, (x + shift) % 4)) for p in (1, 2) for x in range(4)]


def move(value, pairs):
    return lax.ppermute(value, AXES, pairs)


def depth_ring(shift):
    return [(owner(p, x), owner(p, (x + shift) % 4)) for p in range(PANELS) for x in range(4)]


def spread_steps():
    y0, z0 = 1, 0
    y = [("y", 2), ("y", 1), ("y", 3)]
    z = [("z", 4), ("z", 2), ("z", 6)]
    plans = ((y, z, [("z", 1)]), (z, [("z", 1)], y))
    held = [[(0, 0)], [(0, 0)]]
    for stage in range(3):
        moves = []
        new = [[], []]
        for i in range(3):
            pairs = []
            for core in range(2):
                if i >= len(plans[core][stage]):
                    continue
                axis, hop = plans[core][stage][i]
                for dy, dz in held[core]:
                    to = (dy + hop, dz) if axis == "y" else (dy, dz + hop)
                    new[core].append(to)
                    for x in range(4):
                        pairs.append(
                            (
                                device(x, (y0 + dy) % 4, (z0 + dz) % 8, core),
                                device(x, (y0 + to[0]) % 4, (z0 + to[1]) % 8, core),
                            )
                        )
            moves.append(pairs)
        for core in range(2):
            held[core] += new[core]
        yield moves


def everywhere(shift):
    return [((i // 4) * 4 + i % 4, (i // 4) * 4 + (i % 4 + shift) % 4) for i in range(256)]


def partner():
    return [
        (device(x, y, z, c), device(x, y, z, 1 - c))
        for x in range(4)
        for y in range(4)
        for z in range(8)
        for c in range(2)
    ]


def steps(factor, update):
    core = lax.axis_index("row") % 2
    depth = lax.axis_index("depth")
    flat = lax.axis_index(AXES)
    pos = jnp.stack([depth, core, flat * BLK, flat // 4, jnp.minimum(flat // 4, PANELS - 1)])
    pos = pos.astype(jnp.int32)
    quarter, half = K // 4, K // 8

    packed = (4 * BLK + quarter, BLK)
    p0, p1, p2, p3, left_a, left_b = call(
        pack_kernel, 8, [packed] * 4 + [(BLK, B)] * 2, [(K, BLK)], pos, factor, update
    )
    left_a = move(left_a, [(owner(p, x), helper(p, x)) for p in (1, 2) for x in range(4)])
    left_b = move(left_b, [(owner(2, x), helper(2, x)) for x in range(4)])
    parts, lefts = [p0], [left_a]
    for s, p in ((1, p1), (2, p2), (3, p3)):
        parts.append(move(p, depth_ring(s)))
    for s in range(1, 4):
        lefts.append(move(left_a, helper_ring(s)))
    rights = [left_b]
    for s in range(1, 4):
        rights.append(move(left_b, helper_ring(s)[4:]))
    inv, v, g0 = call(
        first_kernel,
        16,
        [jax.ShapeDtypeStruct((3, B, B), jnp.bfloat16), (4, quarter, BLK), (quarter, B)],
        [(4, 4, BLK, BLK)],
        pos,
        *parts,
    )
    got1 = move(g0, [(owner(0, x), helper(1, x)) for x in range(4)])
    g0, got1 = lax.optimization_barrier((g0, got1))
    got2 = move(g0, [(owner(0, x), helper(2, x)) for x in range(4)])
    g0, t = call(
        left0_kernel, 16, [(quarter, B), (4, quarter, BLK)], [], pos, got1, got2, *lefts
    )
    t = move(t, [(helper(p, x), owner(p, x)) for p in (1, 2) for x in range(4)])
    v, g1 = call(second_kernel, 16, [(4, quarter, BLK), (quarter, B)], [], pos, v, t, inv)
    g1 = move(g1, [(owner(1, x), helper(2, x)) for x in range(4)])
    (t,) = call(left1_kernel, 16, [(4, quarter, BLK)], [], pos, g1, *rights)
    t = move(t, [(helper(2, x), owner(2, x)) for x in range(4)])
    keep, send = call(
        third_kernel, 16, [(half, PANELS * B)] * 2, [(4, quarter, BLK)], pos, v, t, inv, g0, g1
    )
    swap = [(owner(2, x), helper(2, x)) for x in range(4)]
    value = keep + move(send, swap + [(b, a) for a, b in swap])
    for moves in spread_steps():
        value = sum([move(value, pairs) for pairs in moves], value)
    mine = [value] + [move(value, everywhere(s)) for s in range(1, 4)]
    others = move(jnp.stack(mine), partner())
    return tuple(last_call(pos, factor, update, *mine, others))


def solution(mesh):
    spec = P(AXES, None)
    return jax.shard_map(
        steps, mesh=mesh, in_specs=(spec, spec), out_specs=(spec, spec), check_vma=False
    )
```

```python
from functools import partial

import jax
import jax.numpy as jnp
from jax import lax
from jax.experimental import pallas as pl
from jax.experimental.pallas import tpu as pltpu
from jax.sharding import PartitionSpec as P


B = 512
K = 256
PANELS = 3
BLK = 128
STEP = 16
NB = 6
AXES = ("row", "col", "depth")
PASSES = 6
SHARE = 16
F32 = jnp.float32


def pieces_of(x):
    terms = []
    for _ in range(2 if PASSES == 3 else 3):
        terms.append(x.astype(jnp.bfloat16))
        x = x - terms[-1].astype(F32)
    return terms


LEFT, RIGHT = ((0, 0, 1), (0, 1, 0)) if PASSES == 3 else ((0, 0, 0, 1, 1, 2), (0, 1, 2, 0, 1, 0))


def product(a, b, da, db):
    a = a if isinstance(a, list) else pieces_of(a)
    b = b if isinstance(b, list) else pieces_of(b)
    a = jnp.concatenate([a[i] for i in LEFT], da)
    b = jnp.concatenate([b[i] for i in RIGHT], db)
    return lax.dot_general(a, b, (((da,), (db,)), ((), ())), preferred_element_type=F32)


def nn(a, b):
    return product(a, b, 1, 0)


def nt(a, b):
    return product(a, b, 1, 1)


def tn(a, b):
    return product(a, b, 0, 0)


def iota(shape, dim):
    return lax.broadcasted_iota(jnp.int32, shape, dim)


def tri_inverse_128(blocks):
    r = iota((BLK, BLK), 0)
    c = iota((BLK, BLK), 1)
    inv = [jnp.where(r == c, 1.0 / jnp.where(r == c, d, 1.0), 0.0) for d in blocks]
    m = 1
    while m < BLK:
        pick = (r // (2 * m) == c // (2 * m)) & (r // m != c // m) & (r > c)
        low = [jnp.where(pick, d, 0.0) for d in blocks]
        if m == 1:
            mid = [jnp.sum(x, axis=0, keepdims=True) for x in inv]
            row = [jnp.sum(x, axis=1, keepdims=True) for x in inv]
            inv = [x - rr * l * mm for x, l, rr, mm in zip(inv, low, row, mid)]
        else:
            half = [nn(l, x) for l, x in zip(low, inv)]
            inv = [x - nn(x, h) for x, h in zip(inv, half)]
        m *= 2
    return inv


def row(x, s):
    return jnp.broadcast_to(x[s : s + 1, :], (8, BLK))


def col(x, c):
    return jnp.broadcast_to(x[:, c : c + 1], (8, BLK))


def cholesky_rows(blocks, j0):
    tiles = range(STEP // 8)
    shape = (8, BLK)
    r = iota(shape, 0)
    lane = iota(shape, 1)
    here = (lane >= j0) & (lane < j0 + STEP)
    x = [[w[8 * v : 8 * v + 8, :] for v in tiles] for w in blocks]
    part = [lane >= SHARE * i for i in range(len(blocks))]
    c = [[None] * (8 * v + 8) for v in tiles]
    for v in tiles:
        for t in range(8 * v + 8):
            both = col(x[0][v], j0 + t)
            for i in range(1, len(blocks)):
                both = jnp.where(part[i], col(x[i][v], j0 + t), both)
            c[v][t] = both
    mult = []
    roots = [None for _ in tiles]
    for t in range(STEP):
        first, s = divmod(t, 8)
        root = lax.rsqrt(row(c[first][t], s))
        recip = root * root
        m = {v: c[v][t] * recip for v in tiles if v >= first}
        m[first] = jnp.where(r > s, m[first], 0.0)
        for u in range(t + 1, STEP):
            y = row(c[u // 8][t], u % 8)
            for v in range(u // 8, len(tiles)):
                c[v][u] = c[v][u] - m[v] * y
        mult.append(m)
        roots[first] = root if s == 0 else jnp.where(r == s, root, roots[first])
    out = []
    for i, w in enumerate(x):
        rest = [jnp.where(here, jnp.where(lane == r + j0 + 8 * v, 1.0, 0.0), w[v]) for v in tiles]
        for t in range(STEP):
            first, s = divmod(t, 8)
            y = row(rest[first], s)
            for v, m in mult[t].items():
                rest[v] = rest[v] - col(m, SHARE * i) * y
        out.append(jnp.concatenate([rest[v] * col(roots[v], SHARE * i) for v in tiles], 0))
    return out


def chol_inverse_128(src, dst, count):
    c = iota((STEP, BLK), 1)
    steps = BLK // STEP
    w = [[src[i, q * STEP : (q + 1) * STEP, :] for q in range(steps)] for i in range(count)]
    for j in range(steps):
        j0 = j * STEP
        done = cholesky_rows([w[i][j] for i in range(count)], j0)
        for i, x in enumerate(done):
            dst[i, j0 : j0 + STEP, :] = jnp.where(c < j0 + STEP, x, 0.0)
            if j + 1 < steps:
                y = tn(x, x)
                here = (c >= j0) & (c < j0 + STEP)
                for q in range(j + 1, steps):
                    w[i][q] = jnp.where(here, 0.0, w[i][q]) - y[q * STEP : (q + 1) * STEP, :]


def call(kernel, mib, outs, scratch, scalars, *arrays):
    smem = pl.BlockSpec(memory_space=pltpu.SMEM)
    vmem = pl.BlockSpec(memory_space=pltpu.VMEM)
    outs = [s if isinstance(s, jax.ShapeDtypeStruct) else jax.ShapeDtypeStruct(s, F32) for s in outs]
    return pl.pallas_call(
        kernel,
        out_shape=outs,
        in_specs=[smem] + [vmem] * len(arrays),
        out_specs=[vmem] * len(outs),
        scratch_shapes=[pltpu.VMEM(s, F32) for s in scratch],
        compiler_params=pltpu.CompilerParams(vmem_limit_bytes=mib * 1024 * 1024),
    )(scalars, *arrays)


def pack_kernel(pos, f, u, p0, p1, p2, p3, left_a, left_b, u_s):
    depth, group = pos[0], pos[4]
    u_s[...] = u[...].T
    start = pl.multiple_of(group * B, B)
    for shift, out in enumerate((p0, p1, p2, p3)):
        for k in range(4):
            out[k * BLK : (k + 1) * BLK, :] = f[:, pl.ds(start + k * BLK, BLK)]
        first = pl.multiple_of(((depth + shift) % 4) * (K // 4), K // 4)
        out[4 * BLK :, :] = u_s[pl.ds(first, K // 4), :]
    left_a[...] = f[:, :B]
    left_b[...] = f[:, B : 2 * B]


def first_kernel(pos, p0, p1, p2, p3, inv_ref, v_ref, g_ref, d_s):
    @pl.when(pos[3] < PANELS)
    def _():
        depth = pos[0]
        for shift, p in enumerate((p0, p1, p2, p3)):
            slot = (depth + 4 - shift) % 4
            d_s[slot] = p[: 4 * BLK, :].reshape(4, BLK, BLK)
            v_ref[slot] = p[4 * BLK :, :]
        diag = tri_inverse_128([d_s[i, i] for i in range(4)])
        low10 = -nn(diag[1], nn(d_s[1, 0], diag[0]))
        low32 = -nn(diag[3], nn(d_s[3, 2], diag[2]))
        zero = jnp.zeros((BLK, BLK), F32)
        top = jnp.concatenate([jnp.concatenate([diag[0], zero], 1), jnp.concatenate([low10, diag[1]], 1)], 0)
        bot = jnp.concatenate([jnp.concatenate([diag[2], zero], 1), jnp.concatenate([low32, diag[3]], 1)], 0)
        below = jnp.concatenate(
            [jnp.concatenate([d_s[i, 0], d_s[i, 1]], 1) for i in (2, 3)], 0
        )
        cross = -nn(bot, nn(below, top))
        inv = jnp.concatenate(
            [
                jnp.concatenate([top, jnp.zeros((2 * BLK, 2 * BLK), F32)], 1),
                jnp.concatenate([cross, bot], 1),
            ],
            0,
        )
        terms = pieces_of(inv)
        for i, x in enumerate(terms):
            inv_ref[i] = x
        v = jnp.concatenate([v_ref[i] for i in range(4)], 1)
        g_ref[...] = nt(v, terms)


def left_product(pos, g, left, out, base=None):
    terms = pieces_of(g)
    for shift, piece in enumerate(left):
        slot = (pos[0] + 4 - shift) % 4
        new = nt(terms, piece[...])
        out[slot] = new if base is None else base[slot] + new


def left_kernel(group, pos, g, l0, l1, l2, l3, out):
    @pl.when(pos[3] == group)
    def _():
        left_product(pos, g[...], (l0, l1, l2, l3), out)


def left_add_kernel(pos, g, t, l0, l1, l2, l3, out):
    @pl.when(pos[3] == 10)
    def _():
        left_product(pos, g[...], (l0, l1, l2, l3), out, t)


def solve(v, t, inv, out):
    for i in range(4):
        out[i] = v[i] - t[i]
    return nt(jnp.concatenate([out[i] for i in range(4)], 1), [inv[i] for i in range(3)])


def second_kernel(pos, v, t, inv, g_ref, v_s):
    @pl.when(pos[3] == 1)
    def _():
        g_ref[...] = solve(v, t, inv, v_s)


def third_kernel(pos, v, t, inv, g0, g1, keep, send, v_s):
    h = K // 8
    mine, theirs = slice(0, h), slice(h, 2 * h)
    owns, helps = pos[3] == 2, pos[3] == 10
    for ref in (keep, send):
        ref[...] = jnp.zeros((h, PANELS * B), F32)

    @pl.when(helps)
    def _():
        for ref, rows in ((keep, theirs), (send, mine)):
            for i, g in enumerate((g0, g1)):
                ref[:, i * B : (i + 1) * B] = g[rows, :]

    @pl.when(owns)
    def _():
        g2 = solve(v, t, inv, v_s)
        keep[:, 2 * B :] = g2[mine]
        send[:, 2 * B :] = g2[theirs]


def last_kernel(pos, f, u, a0, a1, a2, a3, others, f_ref, u_ref, t_s, h_s, s_s, src, dst):
    depth, core, base = pos[0], pos[1], pos[2]
    for shift, mine in enumerate((a0, a1, a2, a3)):
        slot = (depth + 4 - shift) % 4
        t_s[slot * 2 + core] = mine[...]
        t_s[slot * 2 + 1 - core] = others[shift]
    acc = jnp.where(iota((K, K), 0) == iota((K, K), 1), 1.0, 0.0)
    v = u[...]
    for j in range(NB):
        gt = t_s[:, :, j * K : (j + 1) * K].reshape(K, K)
        acc = acc + nt(gt, gt)
        v = v - nt(f[:, j * K : (j + 1) * K], gt)
        for k in range(2):
            sl = slice(k * BLK, (k + 1) * BLK)
            h_s[j, k, 0:K, :] = acc[:, sl]
            h_s[j, k, K : K + BLK, :] = v[:, sl]
        g = gt.T
        if j == 0:
            first = g
        else:
            for k in range(2):
                h_s[j - 1, k, K + BLK :, :] = g[:, k * BLK : (k + 1) * BLK]

    def before(j):
        if j == 0:
            return u[...]
        return jnp.concatenate([h_s[j - 1, k, K : K + BLK, :] for k in range(2)], 1)

    def step(i, carry):
        del carry

        @pl.when(i == 0)
        def _():
            for j in range(NB):
                src[j] = h_s[j, 0, 0:BLK, :]

        chol_inverse_128(src, dst, NB)

        @pl.when(i == 0)
        def _():
            for j in range(NB):
                low = nt(h_s[j, 0, BLK:, :], dst[j])
                h_s[j, 0, BLK:, :] = low
                low = h_s[j, 1, BLK:, :] - nt(low, low[0:BLK, :])
                h_s[j, 1, BLK:, :] = low
                src[j] = low[0:BLK, :]

        @pl.when(i == 1)
        def _():
            for j in range(NB):
                h_s[j, 1, K:, :] = nt(h_s[j, 1, K:, :], dst[j])
            for j in range(NB):
                if j == 0:
                    g = first
                else:
                    g = jnp.concatenate([h_s[j - 1, k, K + BLK :, :] for k in range(2)], 1)
                full = nt(jnp.concatenate([g, before(j)], 0), g)
                eye = jnp.where(iota((K, K), 0) == iota((K, K), 1), 1.0, 0.0)
                s_s[j, 0:K, :] = full[0:K] + eye
                s_s[j, K:, :] = full[K:] + f[:, j * K : (j + 1) * K]
                src[j] = s_s[j, 0:BLK, 0:BLK]

        @pl.when(i == 2)
        def _():
            for j in range(NB):
                low = nt(s_s[j, BLK:, 0:BLK], dst[j])
                s_s[j, BLK:, 0:BLK] = low
                low = s_s[j, BLK:, BLK:] - nt(low, low[0:BLK, :])
                s_s[j, BLK:, BLK:] = low
                src[j] = low[0:BLK, :]

        @pl.when(i == 3)
        def _():
            rows = base + iota((BLK, BLK), 0)
            cols = iota((BLK, BLK), 1)
            for j in range(NB):
                lo = j * K
                f_ref[:, lo : lo + BLK] = jnp.where(rows >= cols + lo, s_s[j, K:, 0:BLK], 0.0)
                lo = lo + BLK
                new = nt(s_s[j, K:, BLK:], dst[j])
                f_ref[:, lo : lo + BLK] = jnp.where(rows >= cols + lo, new, 0.0)

        return 0

    lax.fori_loop(0, 4, step, 0)
    rows = base + iota((BLK, K), 0)
    out = before(2)
    for p in range(1, PANELS):
        out = jnp.where(rows >= p * B, before(2 * p + 2), out)
    u_ref[...] = out


def last_call(pos, factor, update, *pieces):
    return call(
        last_kernel,
        32,
        [factor.shape, update.shape],
        [
            (8, K // 8, PANELS * B),
            (NB, 2, K + BLK + K, BLK),
            (NB, K + BLK, K),
            (NB, BLK, BLK),
            (NB, BLK, BLK),
        ],
        pos,
        factor,
        update,
        *pieces,
    )


def device(x, y, z, core):
    return (((z // 2) * 2 + core) * 8 + y * 2 + z % 2) * 4 + x


def owner(p, x):
    return p * 4 + x


def helper(p, x):
    return (8 + p) * 4 + x


def helper_ring(shift):
    return [(helper(p, x), helper(p, (x + shift) % 4)) for p in (1, 2) for x in range(4)]


def move(value, pairs):
    return lax.ppermute(value, AXES, pairs)


def depth_ring(shift):
    return [(owner(p, x), owner(p, (x + shift) % 4)) for p in range(PANELS) for x in range(4)]


def spread_steps():
    y0, z0 = 1, 0
    y = [("y", 2), ("y", 1), ("y", 3)]
    z = [("z", 4), ("z", 2), ("z", 6)]
    plans = ((y, z, [("z", 1)]), (z, [("z", 1)], y))
    held = [[(0, 0)], [(0, 0)]]
    for stage in range(3):
        moves = []
        new = [[], []]
        for i in range(3):
            pairs = []
            for core in range(2):
                if i >= len(plans[core][stage]):
                    continue
                axis, hop = plans[core][stage][i]
                for dy, dz in held[core]:
                    to = (dy + hop, dz) if axis == "y" else (dy, dz + hop)
                    new[core].append(to)
                    for x in range(4):
                        pairs.append(
                            (
                                device(x, (y0 + dy) % 4, (z0 + dz) % 8, core),
                                device(x, (y0 + to[0]) % 4, (z0 + to[1]) % 8, core),
                            )
                        )
            moves.append(pairs)
        for core in range(2):
            held[core] += new[core]
        yield moves


def everywhere(shift):
    return [((i // 4) * 4 + i % 4, (i // 4) * 4 + (i % 4 + shift) % 4) for i in range(256)]


def partner():
    return [
        (device(x, y, z, c), device(x, y, z, 1 - c))
        for x in range(4)
        for y in range(4)
        for z in range(8)
        for c in range(2)
    ]


def steps(factor, update):
    core = lax.axis_index("row") % 2
    depth = lax.axis_index("depth")
    flat = lax.axis_index(AXES)
    pos = jnp.stack([depth, core, flat * BLK, flat // 4, jnp.minimum(flat // 4, PANELS - 1)])
    pos = pos.astype(jnp.int32)
    quarter, half = K // 4, K // 8

    packed = (4 * BLK + quarter, BLK)
    p0, p1, p2, p3, left_a, left_b = call(
        pack_kernel, 8, [packed] * 4 + [(BLK, B)] * 2, [(K, BLK)], pos, factor, update
    )
    left_a = move(left_a, [(owner(p, x), helper(p, x)) for p in (1, 2) for x in range(4)])
    left_b = move(left_b, [(owner(2, x), helper(2, x)) for x in range(4)])
    parts, lefts = [p0], [left_a]
    for s, p in ((1, p1), (2, p2), (3, p3)):
        parts.append(move(p, depth_ring(s)))
    for s in range(1, 4):
        lefts.append(move(left_a, helper_ring(s)))
    rights = [left_b]
    for s in range(1, 4):
        rights.append(move(left_b, helper_ring(s)[4:]))
    inv, v, g0 = call(
        first_kernel,
        16,
        [jax.ShapeDtypeStruct((3, B, B), jnp.bfloat16), (4, quarter, BLK), (quarter, B)],
        [(4, 4, BLK, BLK)],
        pos,
        *parts,
    )
    got1 = move(g0, [(owner(0, x), helper(1, x)) for x in range(4)])
    g0, got1 = lax.optimization_barrier((g0, got1))
    got2 = move(g0, [(owner(0, x), helper(2, x)) for x in range(4)])
    slots = (4, quarter, BLK)
    (t,) = call(partial(left_kernel, 9), 16, [slots], [], pos, got1, *lefts)
    t = move(t, [(helper(1, x), owner(1, x)) for x in range(4)])
    (g1,) = call(second_kernel, 16, [(quarter, B)], [slots], pos, v, t, inv)
    g1 = move(g1, [(owner(1, x), helper(2, x)) for x in range(4)])
    (t,) = call(partial(left_kernel, 10), 16, [slots], [], pos, got2, *lefts)
    (t,) = call(left_add_kernel, 16, [slots], [], pos, g1, t, *rights)
    t = move(t, [(helper(2, x), owner(2, x)) for x in range(4)])
    keep, send = call(
        third_kernel, 16, [(half, PANELS * B)] * 2, [(4, quarter, BLK)], pos, v, t, inv, got2, g1
    )
    swap = [(owner(2, x), helper(2, x)) for x in range(4)]
    value = keep + move(send, swap + [(b, a) for a, b in swap])
    for moves in spread_steps():
        value = sum([move(value, pairs) for pairs in moves], value)
    mine = [value] + [move(value, everywhere(s)) for s in range(1, 4)]
    others = move(jnp.stack(mine), partner())
    return tuple(last_call(pos, factor, update, *mine, others))


def solution(mesh):
    spec = P(AXES, None)
    return jax.shard_map(
        steps, mesh=mesh, in_specs=(spec, spec), out_specs=(spec, spec), check_vma=False
    )
```

```python
from functools import partial

import jax
import jax.numpy as jnp
from jax import lax
from jax.experimental import pallas as pl
from jax.experimental.pallas import tpu as pltpu
from jax.sharding import PartitionSpec as P


B = 512
K = 256
PANELS = 3
BLK = 128
STEP = 16
NB = 6
AXES = ("row", "col", "depth")
PASSES = 6
SHARE = 16
F32 = jnp.float32


def pieces_of(x):
    terms = []
    for _ in range(2 if PASSES == 3 else 3):
        terms.append(x.astype(jnp.bfloat16))
        x = x - terms[-1].astype(F32)
    return terms


LEFT, RIGHT = ((0, 0, 1), (0, 1, 0)) if PASSES == 3 else ((0, 0, 0, 1, 1, 2), (0, 1, 2, 0, 1, 0))


def product(a, b, da, db):
    a = a if isinstance(a, list) else pieces_of(a)
    b = b if isinstance(b, list) else pieces_of(b)
    a = jnp.concatenate([a[i] for i in LEFT], da)
    b = jnp.concatenate([b[i] for i in RIGHT], db)
    return lax.dot_general(a, b, (((da,), (db,)), ((), ())), preferred_element_type=F32)


def nn(a, b):
    return product(a, b, 1, 0)


def nt(a, b):
    return product(a, b, 1, 1)


def tn(a, b):
    return product(a, b, 0, 0)


def iota(shape, dim):
    return lax.broadcasted_iota(jnp.int32, shape, dim)


def tri_inverse_128(blocks):
    r = iota((BLK, BLK), 0)
    c = iota((BLK, BLK), 1)
    inv = [jnp.where(r == c, 1.0 / jnp.where(r == c, d, 1.0), 0.0) for d in blocks]
    m = 1
    while m < BLK:
        pick = (r // (2 * m) == c // (2 * m)) & (r // m != c // m) & (r > c)
        low = [jnp.where(pick, d, 0.0) for d in blocks]
        if m == 1:
            mid = [jnp.sum(x, axis=0, keepdims=True) for x in inv]
            row = [jnp.sum(x, axis=1, keepdims=True) for x in inv]
            inv = [x - rr * l * mm for x, l, rr, mm in zip(inv, low, row, mid)]
        else:
            half = [nn(l, x) for l, x in zip(low, inv)]
            inv = [x - nn(x, h) for x, h in zip(inv, half)]
        m *= 2
    return inv


def row(x, s):
    return jnp.broadcast_to(x[s : s + 1, :], (8, BLK))


def col(x, c):
    return jnp.broadcast_to(x[:, c : c + 1], (8, BLK))


def cholesky_rows(blocks, j0):
    tiles = range(STEP // 8)
    shape = (8, BLK)
    r = iota(shape, 0)
    lane = iota(shape, 1)
    here = (lane >= j0) & (lane < j0 + STEP)
    x = [[w[8 * v : 8 * v + 8, :] for v in tiles] for w in blocks]
    part = [lane >= SHARE * i for i in range(len(blocks))]
    c = [[None] * (8 * v + 8) for v in tiles]
    for v in tiles:
        for t in range(8 * v + 8):
            both = col(x[0][v], j0 + t)
            for i in range(1, len(blocks)):
                both = jnp.where(part[i], col(x[i][v], j0 + t), both)
            c[v][t] = both
    mult = []
    roots = [None for _ in tiles]
    for t in range(STEP):
        first, s = divmod(t, 8)
        root = lax.rsqrt(row(c[first][t], s))
        recip = root * root
        m = {v: c[v][t] * recip for v in tiles if v >= first}
        m[first] = jnp.where(r > s, m[first], 0.0)
        for u in range(t + 1, STEP):
            y = row(c[u // 8][t], u % 8)
            for v in range(u // 8, len(tiles)):
                c[v][u] = c[v][u] - m[v] * y
        mult.append(m)
        roots[first] = root if s == 0 else jnp.where(r == s, root, roots[first])
    out = []
    for i, w in enumerate(x):
        rest = [jnp.where(here, jnp.where(lane == r + j0 + 8 * v, 1.0, 0.0), w[v]) for v in tiles]
        for t in range(STEP):
            first, s = divmod(t, 8)
            y = row(rest[first], s)
            for v, m in mult[t].items():
                rest[v] = rest[v] - col(m, SHARE * i) * y
        out.append(jnp.concatenate([rest[v] * col(roots[v], SHARE * i) for v in tiles], 0))
    return out


def chol_inverse_128(src, dst, count):
    c = iota((STEP, BLK), 1)
    steps = BLK // STEP
    w = [[src[i, q * STEP : (q + 1) * STEP, :] for q in range(steps)] for i in range(count)]
    for j in range(steps):
        j0 = j * STEP
        done = cholesky_rows([w[i][j] for i in range(count)], j0)
        for i, x in enumerate(done):
            dst[i, j0 : j0 + STEP, :] = jnp.where(c < j0 + STEP, x, 0.0)
            if j + 1 < steps:
                y = tn(x, x)
                here = (c >= j0) & (c < j0 + STEP)
                for q in range(j + 1, steps):
                    w[i][q] = jnp.where(here, 0.0, w[i][q]) - y[q * STEP : (q + 1) * STEP, :]


def call(kernel, mib, outs, scratch, scalars, *arrays):
    smem = pl.BlockSpec(memory_space=pltpu.SMEM)
    vmem = pl.BlockSpec(memory_space=pltpu.VMEM)
    outs = [s if isinstance(s, jax.ShapeDtypeStruct) else jax.ShapeDtypeStruct(s, F32) for s in outs]
    return pl.pallas_call(
        kernel,
        out_shape=outs,
        in_specs=[smem] + [vmem] * len(arrays),
        out_specs=[vmem] * len(outs),
        scratch_shapes=[pltpu.VMEM(s, F32) for s in scratch],
        compiler_params=pltpu.CompilerParams(vmem_limit_bytes=mib * 1024 * 1024),
    )(scalars, *arrays)


def pack_kernel(pos, f, u, own, up, down, left_a, left_b, u_s):
    depth, group = pos[0], pos[4]
    u_s[...] = u[...].T
    start = pl.multiple_of(group * B, B)
    quarter, half, h = K // 4, K // 8, 2 * BLK

    def cut(k):
        return f[:, pl.ds(start + k * BLK, BLK)]

    def update_rows(shift, first, size):
        at = pl.multiple_of(((depth + shift) % 4) * quarter + first, size)
        return u_s[pl.ds(at, size), :]

    for out, order, shift, first in ((up, (0, 1, 2, 3), 1, 0), (down, (2, 3, 0, 1), 3, half)):
        out[0:BLK, :] = cut(order[0])
        out[BLK:h, :] = cut(order[1])
        out[h : h + half, :] = update_rows(2, first, half)
        out[h + half : h + half + BLK, :] = cut(order[2])
        out[h + half + BLK : 2 * h + half, :] = cut(order[3])
        out[2 * h + half :, :] = update_rows(shift, 0, quarter)
    for k in range(4):
        own[k * BLK : (k + 1) * BLK, :] = cut(k)
    own[2 * h :, :] = update_rows(0, 0, quarter)
    left_a[...] = f[:, :B]
    left_b[...] = f[:, B : 2 * B]


def first_kernel(pos, own, low, high, far_low, far_high, inv_ref, v_ref, g_ref, d_s):
    @pl.when(pos[3] < PANELS)
    def _():
        depth = pos[0]
        h, half = 2 * BLK, K // 8
        two = (2, BLK, BLK)
        d_s[depth] = own[: 2 * h, :].reshape(4, BLK, BLK)
        v_ref[depth] = own[2 * h :, :]
        for p, slot, lead in ((low, (depth + 3) % 4, 0), (high, (depth + 1) % 4, 2)):
            d_s[slot, lead : lead + 2] = p[:h, :].reshape(two)
            d_s[slot, 2 - lead : 4 - lead] = p[h + half : 2 * h + half, :].reshape(two)
            v_ref[slot] = p[2 * h + half :, :]
        slot = (depth + 2) % 4
        for p, lead, first in ((far_low, 0, 0), (far_high, 2, half)):
            d_s[slot, lead : lead + 2] = p[:h, :].reshape(two)
            v_ref[slot, first : first + half, :] = p[h:, :]
        diag = tri_inverse_128([d_s[i, i] for i in range(4)])
        low10 = -nn(diag[1], nn(d_s[1, 0], diag[0]))
        low32 = -nn(diag[3], nn(d_s[3, 2], diag[2]))
        zero = jnp.zeros((BLK, BLK), F32)
        top = jnp.concatenate([jnp.concatenate([diag[0], zero], 1), jnp.concatenate([low10, diag[1]], 1)], 0)
        bot = jnp.concatenate([jnp.concatenate([diag[2], zero], 1), jnp.concatenate([low32, diag[3]], 1)], 0)
        below = jnp.concatenate(
            [jnp.concatenate([d_s[i, 0], d_s[i, 1]], 1) for i in (2, 3)], 0
        )
        cross = -nn(bot, nn(below, top))
        inv = jnp.concatenate(
            [
                jnp.concatenate([top, jnp.zeros((2 * BLK, 2 * BLK), F32)], 1),
                jnp.concatenate([cross, bot], 1),
            ],
            0,
        )
        terms = pieces_of(inv)
        for i, x in enumerate(terms):
            inv_ref[i] = x
        v = jnp.concatenate([v_ref[i] for i in range(4)], 1)
        g_ref[...] = nt(v, terms)


def left_product(pos, g, left, out, base=None):
    terms = pieces_of(g)
    for shift, piece in enumerate(left):
        slot = (pos[0] + 4 - shift) % 4
        new = nt(terms, piece[...])
        out[slot] = new if base is None else base[slot] + new


def left_kernel(group, pos, g, l0, l1, l2, l3, out):
    @pl.when(pos[3] == group)
    def _():
        left_product(pos, g[...], (l0, l1, l2, l3), out)


def left_add_kernel(pos, g, t, l0, l1, l2, l3, out):
    @pl.when(pos[3] == 10)
    def _():
        left_product(pos, g[...], (l0, l1, l2, l3), out, t)


def solve(v, t, inv, out):
    for i in range(4):
        out[i] = v[i] - t[i]
    return nt(jnp.concatenate([out[i] for i in range(4)], 1), [inv[i] for i in range(3)])


def second_kernel(pos, v, t, inv, g_ref, v_s):
    @pl.when(pos[3] == 1)
    def _():
        g_ref[...] = solve(v, t, inv, v_s)


def third_kernel(pos, v, t, inv, g0, g1, keep, send, v_s):
    h = K // 8
    mine, theirs = slice(0, h), slice(h, 2 * h)
    owns, helps = pos[3] == 2, pos[3] == 10
    for ref in (keep, send):
        ref[...] = jnp.zeros((h, PANELS * B), F32)

    @pl.when(helps)
    def _():
        for ref, rows in ((keep, theirs), (send, mine)):
            for i, g in enumerate((g0, g1)):
                ref[:, i * B : (i + 1) * B] = g[rows, :]

    @pl.when(owns)
    def _():
        g2 = solve(v, t, inv, v_s)
        keep[:, 2 * B :] = g2[mine]
        send[:, 2 * B :] = g2[theirs]


def last_kernel(pos, f, u, mine, others, f_ref, u_ref, t_s, h_s, s_s, src, dst):
    depth, core, base = pos[0], pos[1], pos[2]
    for shift in range(4):
        slot = (depth + 4 - shift) % 4
        t_s[slot * 2 + core] = mine[shift]
        t_s[slot * 2 + 1 - core] = others[shift]
    acc = jnp.where(iota((K, K), 0) == iota((K, K), 1), 1.0, 0.0)
    v = u[...]
    for j in range(NB):
        gt = t_s[:, :, j * K : (j + 1) * K].reshape(K, K)
        acc = acc + nt(gt, gt)
        v = v - nt(f[:, j * K : (j + 1) * K], gt)
        for k in range(2):
            sl = slice(k * BLK, (k + 1) * BLK)
            h_s[j, k, 0:K, :] = acc[:, sl]
            h_s[j, k, K : K + BLK, :] = v[:, sl]
        g = gt.T
        if j == 0:
            first = g
        else:
            for k in range(2):
                h_s[j - 1, k, K + BLK :, :] = g[:, k * BLK : (k + 1) * BLK]

    def before(j):
        if j == 0:
            return u[...]
        return jnp.concatenate([h_s[j - 1, k, K : K + BLK, :] for k in range(2)], 1)

    def step(i, carry):
        del carry

        @pl.when(i == 0)
        def _():
            for j in range(NB):
                src[j] = h_s[j, 0, 0:BLK, :]

        chol_inverse_128(src, dst, NB)

        @pl.when(i == 0)
        def _():
            for j in range(NB):
                low = nt(h_s[j, 0, BLK:, :], dst[j])
                h_s[j, 0, BLK:, :] = low
                low = h_s[j, 1, BLK:, :] - nt(low, low[0:BLK, :])
                h_s[j, 1, BLK:, :] = low
                src[j] = low[0:BLK, :]

        @pl.when(i == 1)
        def _():
            for j in range(NB):
                h_s[j, 1, K:, :] = nt(h_s[j, 1, K:, :], dst[j])
            for j in range(NB):
                if j == 0:
                    g = first
                else:
                    g = jnp.concatenate([h_s[j - 1, k, K + BLK :, :] for k in range(2)], 1)
                full = nt(jnp.concatenate([g, before(j)], 0), g)
                eye = jnp.where(iota((K, K), 0) == iota((K, K), 1), 1.0, 0.0)
                s_s[j, 0:K, :] = full[0:K] + eye
                s_s[j, K:, :] = full[K:] + f[:, j * K : (j + 1) * K]
                src[j] = s_s[j, 0:BLK, 0:BLK]

        @pl.when(i == 2)
        def _():
            for j in range(NB):
                low = nt(s_s[j, BLK:, 0:BLK], dst[j])
                s_s[j, BLK:, 0:BLK] = low
                low = s_s[j, BLK:, BLK:] - nt(low, low[0:BLK, :])
                s_s[j, BLK:, BLK:] = low
                src[j] = low[0:BLK, :]

        @pl.when(i == 3)
        def _():
            rows = base + iota((BLK, BLK), 0)
            cols = iota((BLK, BLK), 1)
            for j in range(NB):
                lo = j * K
                f_ref[:, lo : lo + BLK] = jnp.where(rows >= cols + lo, s_s[j, K:, 0:BLK], 0.0)
                lo = lo + BLK
                new = nt(s_s[j, K:, BLK:], dst[j])
                f_ref[:, lo : lo + BLK] = jnp.where(rows >= cols + lo, new, 0.0)

        return 0

    lax.fori_loop(0, 4, step, 0)
    rows = base + iota((BLK, K), 0)
    out = before(2)
    for p in range(1, PANELS):
        out = jnp.where(rows >= p * B, before(2 * p + 2), out)
    u_ref[...] = out


def last_call(pos, factor, update, *pieces):
    return call(
        last_kernel,
        32,
        [factor.shape, update.shape],
        [
            (8, K // 8, PANELS * B),
            (NB, 2, K + BLK + K, BLK),
            (NB, K + BLK, K),
            (NB, BLK, BLK),
            (NB, BLK, BLK),
        ],
        pos,
        factor,
        update,
        *pieces,
    )


def device(x, y, z, core):
    return (((z // 2) * 2 + core) * 8 + y * 2 + z % 2) * 4 + x


def owner(p, x):
    return p * 4 + x


def helper(p, x):
    return (8 + p) * 4 + x


def helper_ring(shift):
    return [(helper(p, x), helper(p, (x + shift) % 4)) for p in (1, 2) for x in range(4)]


def move(value, pairs):
    return lax.ppermute(value, AXES, pairs)


def depth_ring(shift):
    return [(owner(p, x), owner(p, (x + shift) % 4)) for p in range(PANELS) for x in range(4)]


def spread_steps():
    y0, z0 = 1, 0
    y = [("y", 2), ("y", 1), ("y", 3)]
    z = [("z", 4), ("z", 2), ("z", 6)]
    plans = ((y, z, [("z", 1)]), (z, [("z", 1)], y))
    held = [[(0, 0)], [(0, 0)]]
    for stage in range(3):
        moves = []
        new = [[], []]
        for i in range(3):
            pairs = []
            for core in range(2):
                if i >= len(plans[core][stage]):
                    continue
                axis, hop = plans[core][stage][i]
                for dy, dz in held[core]:
                    to = (dy + hop, dz) if axis == "y" else (dy, dz + hop)
                    new[core].append(to)
                    for x in range(4):
                        pairs.append(
                            (
                                device(x, (y0 + dy) % 4, (z0 + dz) % 8, core),
                                device(x, (y0 + to[0]) % 4, (z0 + to[1]) % 8, core),
                            )
                        )
            moves.append(pairs)
        for core in range(2):
            held[core] += new[core]
        yield moves


def everywhere(shift):
    return [((i // 4) * 4 + i % 4, (i // 4) * 4 + (i % 4 + shift) % 4) for i in range(256)]


def partner():
    return [
        (device(x, y, z, c), device(x, y, z, 1 - c))
        for x in range(4)
        for y in range(4)
        for z in range(8)
        for c in range(2)
    ]


def steps(factor, update):
    core = lax.axis_index("row") % 2
    depth = lax.axis_index("depth")
    flat = lax.axis_index(AXES)
    pos = jnp.stack([depth, core, flat * BLK, flat // 4, jnp.minimum(flat // 4, PANELS - 1)])
    pos = pos.astype(jnp.int32)
    quarter, half = K // 4, K // 8

    rows = 4 * BLK + quarter
    own, up, down, left_a, left_b = call(
        pack_kernel,
        8,
        [(rows, BLK), (rows + half, BLK), (rows + half, BLK), (BLK, B), (BLK, B)],
        [(K, BLK)],
        pos,
        factor,
        update,
    )
    left_a = move(left_a, [(owner(p, x), helper(p, x)) for p in (1, 2) for x in range(4)])
    left_b = move(left_b, [(owner(2, x), helper(2, x)) for x in range(4)])
    lefts = [left_a]
    low = move(up, depth_ring(1))
    high = move(down, depth_ring(3))
    part = 2 * BLK + half
    far_low = move(low[:part], depth_ring(1))
    far_high = move(high[:part], depth_ring(3))
    for s in range(1, 4):
        lefts.append(move(left_a, helper_ring(s)))
    rights = [left_b]
    for s in range(1, 4):
        rights.append(move(left_b, helper_ring(s)[4:]))
    inv, v, g0 = call(
        first_kernel,
        16,
        [jax.ShapeDtypeStruct((3, B, B), jnp.bfloat16), (4, quarter, BLK), (quarter, B)],
        [(4, 4, BLK, BLK)],
        pos,
        own,
        low,
        high,
        far_low,
        far_high,
    )
    got1 = move(g0, [(owner(0, x), helper(1, x)) for x in range(4)])
    g0, got1 = lax.optimization_barrier((g0, got1))
    got2 = move(g0, [(owner(0, x), helper(2, x)) for x in range(4)])
    slots = (4, quarter, BLK)
    (t,) = call(partial(left_kernel, 9), 16, [slots], [], pos, got1, *lefts)
    t = move(t, [(helper(1, x), owner(1, x)) for x in range(4)])
    (g1,) = call(second_kernel, 16, [(quarter, B)], [slots], pos, v, t, inv)
    g1 = move(g1, [(owner(1, x), helper(2, x)) for x in range(4)])
    (t,) = call(partial(left_kernel, 10), 16, [slots], [], pos, got2, *lefts)
    (t,) = call(left_add_kernel, 16, [slots], [], pos, g1, t, *rights)
    t = move(t, [(helper(2, x), owner(2, x)) for x in range(4)])
    keep, send = call(
        third_kernel, 16, [(half, PANELS * B)] * 2, [(4, quarter, BLK)], pos, v, t, inv, got2, g1
    )
    swap = [(owner(2, x), helper(2, x)) for x in range(4)]
    value = keep + move(send, swap + [(b, a) for a, b in swap])
    for moves in spread_steps():
        value = sum([move(value, pairs) for pairs in moves], value)
    low, high = move(value, everywhere(1)), move(value, everywhere(3))
    far = [move(low[: half // 2], everywhere(1)), move(high[half // 2 :], everywhere(3))]
    mine = jnp.stack([value, low, jnp.concatenate(far, 0), high])
    others = move(mine, partner())
    return tuple(last_call(pos, factor, update, mine, others))


def solution(mesh):
    spec = P(AXES, None)
    return jax.shard_map(steps, mesh=mesh, in_specs=(spec, spec), out_specs=(spec, spec), check_vma=False)
```
